32 devices in a mesh: section: 2 (over x), expert: 16 (over z, y, core).
Axes of the slice: x: 2, y: 2, z: 4, core: 2. Of those that a mesh axis runs over, the one named last changes fastest.
Arguments:
- hidden_in: bfloat16 [2, 128, 3584], P(None, 'expert'), may hold values from -6 to 6
- layer_gain: float32 [2, 3584], P('section'), may hold values from 0.25 to 1.75
- router: bfloat16 [2, 3584, 4], P('section'), may hold values from -0.09375 to 0.09375
- w_gate: bfloat16 [2, 3584, 8192], P('section', None, 'expert'), may hold values from -0.09375 to 0.09375
- w_up: bfloat16 [2, 3584, 8192], P('section', None, 'expert'), may hold values from -0.09375 to 0.09375
- w_down: bfloat16 [2, 8192, 3584], P('section', 'expert'), may hold values from -0.125 to 0.125
- final_gain: float32 [3584], replicated, may hold values from 0.25 to 1.75
- head: bfloat16 [8192, 3584], P(('section', 'expert')), may hold values from -18.775102 to 18.775102
- routing: int32 [2, 2, 128, 2], P('section', None, 'expert'), may hold values from 0 to 3, all different within a row; in each aligned block of 8 rows (0 to 7, 8 to 15, ..., all dimensions but the last counted through in order) at most 4 rows name the same one
- targets: int32 [2, 128], replicated, may hold values from 0 to 8191
- seq_ids: int32 [2, 128], replicated, may hold values from 0 to 3, never falling along the last dimension, each value on 1 to 64 neighbouring positions
Outputs:
- token_logprob: float32 [2, 128], P(None, 'expert')
- seq_mean: float32 [2, 4], replicated
The draws below stay inside these ranges and needn't reach their ends.
Inputs may be any that keep to these rules, and one draw needn't show every extreme that they name: `routing`: in each aligned block of 8 tokens (the tokens of one device) a token's 2 experts differ and no expert is named by more than 4 tokens; some expert is named by exactly 4. `seq_ids`: ids never fall along a micro-batch's tokens; each of the 4 ids occurs on 1 to 64 tokens, one on exactly 64.
All inputs are finite; a program needn't handle non-finite values.
Results may differ from the reference program's by a relative error of at most 0.014.
Values may be sent and summed in bfloat16 or wider, within the bound.
No kernel may reach another device: no remote copies, remote signals or barrier semaphores. Data moves between devices by JAX's collectives and lax.ppermute only.
A program may use at most 64 MiB of HBM per device.

```python
import math
import jax
import jax.numpy as jnp
import numpy as np
from jax import lax

D = 3584
FF = 2048
FF_SPLIT = 4
TOP = 2
TOK_DEV = 8
MICRO = 2
SEQS = 4
LAYERS = 2
EXPERTS = 4
FF_DEV = 512
TOKENS = 128
VOCAB = 8192
CAP = 4
SEQ_MOST = 64
N_EXPERT = 16


def draw_head(key, part):
    keys = jax.random.split(jax.random.fold_in(key, 17), 2)
    base = jnp.clip(jax.random.normal(keys[0], (VOCAB, D), jnp.float32), -4.0, 4.0)
    position = jnp.arange(VOCAB, dtype=jnp.float32)[:, None] / VOCAB
    rising = 0.6 + 1.2 * position
    jitter = jax.random.uniform(keys[1], (VOCAB, 1), jnp.float32, 0.7, 1.3)
    values = base * (3.0 / math.sqrt(D)) * rising * jitter
    return values.astype(jnp.bfloat16)


def plant(array, rng, low, top_value):
    longest = array.shape.index(max(array.shape))
    spots = []
    for shift in (0, 1):
        where = [jax.random.randint(jax.random.fold_in(rng, axis), (), 0, length) for axis, length in enumerate(array.shape)]
        where[longest] = (where[longest] + shift) % array.shape[longest]
        spots.append(tuple(where))
    return array.at[spots[0]].set(low).at[spots[1]].set(top_value)


def block_scale(own_key, dims, cuts, low, high):
    level = 1.0
    for dim, blocks in cuts:
        steps = jax.random.uniform(jax.random.fold_in(jax.random.fold_in(own_key, 6), dim), (blocks,), jnp.float32, low / len(cuts), high / len(cuts))
        level = level * jnp.repeat(jnp.exp(steps), dims[dim] // blocks).reshape((-1,) + (1,) * (len(dims) - 1 - dim))
    return level


def cumulative_ranks(number_of, lean):
    loads = [(1 << 20) // math.isqrt(rank ** lean) + 1 for rank in range(1, number_of + 1)]
    deviation = 1 + sum(loads) // (1 << 30)
    return np.cumsum(np.array([max(1, weight // deviation) for weight in loads]))


def ranked(own_key, shape, number_of, slope):
    grid = cumulative_ranks(number_of, slope)
    pick = jax.random.randint(jax.random.fold_in(own_key, 1), shape, 0, int(grid[number_of - 1]))
    grade = jnp.searchsorted(jnp.asarray(grid, jnp.int32), pick, side="right")
    return jax.random.permutation(jax.random.fold_in(own_key, 2), number_of)[grade].astype(jnp.int32)


def split_up(amount, total, most, lean):
    loads = [(1 << 20) // math.isqrt(grade ** lean) + 1 for grade in range(2, amount + 1)]
    surplus, holding = total - most - (amount - 1), [1] * (amount - 1)
    while surplus > 0:
        movable = [i for i in range(amount - 1) if holding[i] < most]
        whole, left = sum([loads[i] for i in movable]), surplus
        for i in movable:
            extra = min(most - holding[i], max(1, left * loads[i] // whole), surplus)
            holding[i] = holding[i] + extra
            surplus = surplus - extra
    return np.array([most] + holding)


def ragged(rng, number_of, total, reach, skew):
    if number_of == 2:
        one = jax.random.randint(rng, (), max(1, total - reach), min(reach, total - 1) + 1)
        return jnp.stack([one, total - one])
    lengths = jnp.asarray(split_up(number_of, total, reach, skew), jnp.int32)
    twos = (number_of - 1) // 2
    giver, taker = lengths[1:1 + 2 * twos:2], lengths[2:2 + 2 * twos:2]
    slack = jnp.minimum(giver - 1, reach - taker)
    shifted = jax.random.randint(jax.random.fold_in(rng, 1), (twos,), 0, 1 << 20) % (slack + 1)
    lengths = lengths.at[1:1 + 2 * twos:2].set(giver - shifted).at[2:2 + 2 * twos:2].set(taker + shifted)
    return lengths[jax.random.permutation(jax.random.fold_in(rng, 2), number_of)]


def routed_block(key, own, number, rows, number_of, top, most, slope):
    order = jax.random.permutation(key, number_of)
    heavy_load, common = portions_of(number_of, rows * top, most, slope, True), portions_of(number_of, rows * top, most, slope, False)
    places = jnp.arange(number_of)

    def named(lengths, rotation):
        used = int((lengths > 0).sum())
        fixed = max(1, used // 4)
        shifted = fixed + (places - fixed + rotation * (used - fixed)) % max(1, number_of - fixed)
        return jnp.zeros((number_of,), jnp.int32).at[order[jnp.where(places < fixed, places, shifted)]].set(jnp.asarray(lengths, jnp.int32))

    lengths = jnp.where(number % 4 == 0, named(heavy_load, number // 4), named(common, number - number // 4 - 1))
    mixed = jax.random.permutation(jax.random.fold_in(own, 3), number_of)
    source_of, receiver = mixed[0:number_of // 2 * 2:2], mixed[1:number_of // 2 * 2:2]
    slack = jnp.minimum(lengths[source_of] - 1, most - lengths[receiver]) // 2
    slack = jnp.where((source_of == order[0]) | (receiver == order[0]) | (lengths[receiver] == 0), 0, jnp.maximum(slack, 0))
    shifted = jax.random.randint(jax.random.fold_in(own, 4), (number_of // 2,), 0, 1 << 20) % (slack + 1)
    lengths = lengths.at[source_of].add(-shifted).at[receiver].add(shifted)
    labels = jnp.searchsorted(jnp.cumsum(lengths), jnp.arange(rows * top), side="right").astype(jnp.int32)
    grid = labels.reshape(top, rows).T
    grid = grid[jax.random.permutation(jax.random.fold_in(own, 1), rows)]
    rotation = jax.random.randint(jax.random.fold_in(own, 2), (rows, 1), 0, top)
    return jnp.take_along_axis(grid, (jnp.arange(top)[None, :] + rotation) % top, axis=1)


def portions_of(count, total, most, slope, full):
    loads = [(1 << 20) // math.isqrt(standing ** slope) + 1 for standing in range(1, count + 1)]
    largest = most if full else min(most, max(-(-total // count), total * loads[0] // sum(loads)))
    least = 1 if total - largest >= count - 1 else 0
    given, rest = [largest] + [least] * (count - 1), total - largest - least * (count - 1)
    while rest > 0:
        candidates = [i for i in range(1, count) if given[i] < largest] or [i for i in range(1, count) if given[i] < most]
        mass, left = sum([loads[i] for i in candidates]), rest
        for i in candidates:
            extra = min(most - given[i], max(1, left * loads[i] // mass), rest)
            given[i] = given[i] + extra
            rest = rest - extra
    return np.array(given)


def noise(key, extent, width, bound, cuts=(), held_as=jnp.bfloat16):
    level = block_scale(key, extent, cuts, -0.22, 0.18) if cuts else 1.0
    result = jax.random.normal(key, extent, jnp.float32) * width * level
    return jnp.minimum(jnp.maximum(result, -bound), bound).astype(held_as)


def setup_inputs(seed: int = 0) -> dict:
    streams_of = jax.random.split(jax.random.key(seed), 12)
    hidden_in = noise(streams_of[0], (MICRO, TOKENS, D), 1.0, 6.0, ((1, 16),))
    layer_gain = jnp.clip(1.0 + 0.15 * jax.random.normal(streams_of[1], (LAYERS, D), jnp.float32), 0.25, 1.75)
    router = noise(streams_of[2], (LAYERS, D, EXPERTS), D ** -0.5, 0.09375, ((0, 2),))
    w_gate = noise(streams_of[3], (LAYERS, D, EXPERTS * FF), D ** -0.5, 0.09375, ((0, 2), (2, 16)))
    w_up = noise(streams_of[4], (LAYERS, D, EXPERTS * FF), D ** -0.5, 0.09375, ((0, 2), (2, 16)))
    w_down = noise(streams_of[5], (LAYERS, EXPERTS * FF, D), FF ** -0.5, 0.125, ((0, 2), (1, 16)))
    final_gain = jnp.clip(1.0 + 0.15 * jax.random.normal(streams_of[6], (D,), jnp.float32), 0.25, 1.75)
    head = draw_head(jax.random.fold_in(streams_of[11], 71), 0)
    routing_keys = jax.random.split(jax.random.fold_in(streams_of[8], 1), LAYERS * MICRO * TOKENS // TOK_DEV)
    routing_turns = jax.random.permutation(jax.random.fold_in(streams_of[8], 3), LAYERS * MICRO * TOKENS // TOK_DEV)
    routing = jax.vmap(lambda own, number: routed_block(jax.random.fold_in(streams_of[8], 2), own, number, TOK_DEV, EXPERTS, TOP, CAP, 2))(routing_keys, routing_turns).reshape((LAYERS, MICRO, TOKENS, TOP))
    targets = plant(ranked(streams_of[9], (MICRO, TOKENS), VOCAB, 2), jax.random.fold_in(streams_of[9], 3), 0, VOCAB - 1).astype(jnp.int32)
    seq_ids = jax.vmap(lambda own: jnp.searchsorted(jnp.cumsum(ragged(own, SEQS, TOKENS, SEQ_MOST, 1)), jnp.arange(TOKENS), side="right"))(jax.random.split(streams_of[10], MICRO)).reshape((MICRO, TOKENS)).astype(jnp.int32)
    return dict(hidden_in=hidden_in, layer_gain=layer_gain, router=router, w_gate=w_gate, w_up=w_up, w_down=w_down, final_gain=final_gain, head=head, routing=routing, targets=targets, seq_ids=seq_ids)


def rms_scale(states, gain):
    values = states.astype(jnp.float32)
    factor = lax.rsqrt(lax.optimization_barrier(jnp.mean(values * values, -1, keepdims=True)) + 1e-06)
    return values * factor * gain.astype(jnp.float32)

def run_expert(operands):
    packed_rows, gate_cols, up_cols, down_rows = operands
    gate_val = jnp.dot(packed_rows, gate_cols, preferred_element_type=jnp.float32)
    up_val = jnp.dot(packed_rows, up_cols, preferred_element_type=jnp.float32)
    inner = (jax.nn.silu(gate_val) * up_val).astype(jnp.bfloat16)
    count = inner.shape[0]
    pieces = jnp.einsum('rfk,fkd->rfd', inner.reshape(count, FF_SPLIT, FF_DEV).astype(jnp.float32), down_rows.reshape(FF_SPLIT, FF_DEV, D).astype(jnp.float32), precision=lax.Precision.HIGHEST)
    rounded = lax.optimization_barrier(pieces.astype(jnp.bfloat16))
    return lax.optimization_barrier(jnp.sum(rounded.astype(jnp.float32), 1))

def pick_rows(block_out, slot_index):
    return block_out[slot_index]

def expert_layer(states, gain, router, gate_w, up_w, down_w, route_ids):
    blocks = N_EXPERT
    normed = rms_scale(states, gain).astype(jnp.bfloat16)
    logits = jnp.dot(normed, router, preferred_element_type=jnp.float32)
    chosen = route_ids[:, :, None] == jnp.arange(EXPERTS, dtype=jnp.int32)[None, None, :]
    affinity = jax.nn.sigmoid(lax.optimization_barrier(jnp.sum(jnp.where(chosen, logits[:, None, :], 0.0), -1)))
    weight = affinity / lax.optimization_barrier(jnp.sum(affinity, -1, keepdims=True))
    flags = chosen.reshape(blocks, TOK_DEV * TOP, EXPERTS).astype(jnp.int32)
    ranks = jnp.cumsum(flags, 1) - flags
    slot_ids = lax.optimization_barrier(jnp.sum(ranks * flags, -1)).reshape(blocks, TOK_DEV, TOP)
    target_slot = (route_ids.reshape(blocks, TOK_DEV, TOP) * CAP + slot_ids).astype(jnp.int32)
    places = jnp.arange(EXPERTS * CAP, dtype=jnp.int32)
    table = jnp.any(places[None, :, None, None] == target_slot[:, None], -1).astype(jnp.float32)
    packed = jnp.einsum('bst,btd->bsd', table, normed.reshape(blocks, TOK_DEV, D).astype(jnp.float32), precision=lax.Precision.HIGHEST).astype(jnp.bfloat16)
    per_expert = packed.reshape(blocks, EXPERTS, CAP, D).transpose(1, 0, 2, 3).reshape(EXPERTS, blocks * CAP, D)
    gate_e = gate_w.reshape(D, EXPERTS, FF).transpose(1, 0, 2)
    up_e = up_w.reshape(D, EXPERTS, FF).transpose(1, 0, 2)
    down_e = down_w.reshape(EXPERTS, FF, D)
    outputs = lax.map(run_expert, (per_expert, gate_e, up_e, down_e))
    by_block = outputs.reshape(EXPERTS, blocks, CAP, D).transpose(1, 0, 2, 3).reshape(blocks, EXPERTS * CAP, D)
    picked = jax.vmap(pick_rows)(by_block, target_slot)
    mixed = lax.optimization_barrier(jnp.sum(weight.reshape(blocks, TOK_DEV, TOP)[..., None] * picked, 2)).reshape(TOKENS, D)
    return (states.astype(jnp.float32) + 2.5 * mixed).astype(jnp.bfloat16)

def reference(hidden_in, layer_gain, router, w_gate, w_up, w_down, final_gain, head, routing, targets, seq_ids):
    states = [hidden_in[micro_id] for micro_id in range(MICRO)]
    for level in range(LAYERS):
        states = [expert_layer(states[micro_id], layer_gain[level], router[level], w_gate[level], w_up[level], w_down[level], routing[level, micro_id]) for micro_id in range(MICRO)]
    stacked = jnp.stack(states)
    normed = rms_scale(stacked, final_gain).astype(jnp.bfloat16).reshape(MICRO * TOKENS, D)
    logits = jnp.dot(normed, head.T, preferred_element_type=jnp.float32).reshape(MICRO, TOKENS, VOCAB)
    peak = lax.optimization_barrier(jnp.max(logits, -1))
    total = lax.optimization_barrier(jnp.sum(jnp.exp(logits - peak[..., None]), -1))
    target_logit = jnp.take_along_axis(logits, targets[..., None].astype(jnp.int32), -1)[..., 0]
    logprob = target_logit - (peak + jnp.log(total))
    member = seq_ids[:, :, None] == jnp.arange(SEQS, dtype=jnp.int32)[None, None, :]
    sums = lax.optimization_barrier(jnp.sum(jnp.where(member, logprob[..., None], 0.0), 1))
    counts = lax.optimization_barrier(jnp.sum(member.astype(jnp.float32), 1))
    return (logprob, sums / counts)
```

```python
import jax
import jax.numpy as jnp
from jax import lax
from jax.sharding import PartitionSpec as P


SEQS = 4
PAIR = 2


def rms_scale(states, gain):
    values = states.astype(jnp.float32)
    factor = lax.rsqrt(jnp.mean(values * values, -1, keepdims=True) + 1e-06)
    return values * factor * gain


def body(
    hidden_in, layer_gain, router, w_gate, w_up, w_down, final_gain, head, routing, targets, seq_ids
):
    micro, toks, width = hidden_in.shape
    experts = router.shape[2]
    tops = routing.shape[3]
    sections = lax.axis_size("section")
    members = lax.axis_size("expert")
    section_pos = lax.axis_index("section")
    member_pos = lax.axis_index("expert")
    splits = members // experts
    halves = splits // PAIR
    groups = members // PAIR
    cap = min(toks, 9 * toks * tops // (8 * experts))
    parity = member_pos % PAIR
    same_core = [[g * PAIR + c for g in range(groups)] for c in range(PAIR)]
    partner = [(i, i ^ 1) for i in range(members)]

    def exchange(rows):
        return lax.all_to_all(
            rows, "expert", split_axis=0, concat_axis=0, axis_index_groups=same_core, tiled=True
        )

    def swap_core(rows):
        return lax.ppermute(rows, "expert", partner)

    head_blocks = [head]
    for shift in range(1, micro):
        ring = [(s, s - s % micro + (s + shift) % micro) for s in range(sections)]
        head_blocks.append(lax.ppermute(head, "section", ring))
    batch_pos = section_pos % micro

    route = routing[0].reshape(micro, toks * tops)
    same = route[:, :, None] == route[:, None, :]
    order = jnp.arange(toks * tops)
    slot = jnp.sum(jnp.where(same & (order[None, None, :] < order[None, :, None]), 1, 0), -1)
    batch_ids = jnp.arange(micro, dtype=jnp.int32)[:, None]
    place = ((route * micro + batch_ids) * cap + slot).reshape(micro * toks, tops)
    row = jnp.arange(experts * halves * micro * cap, dtype=jnp.int32)
    per_expert = micro * cap
    row_place = row // (halves * per_expert) * per_expert + row % per_expert
    hit = place[:, :, None] == row_place[None, None, :]
    pack = jnp.any(hit, 1).astype(jnp.bfloat16).T
    chosen = routing[0].reshape(micro * toks, tops)[:, :, None] == jnp.arange(experts, dtype=jnp.int32)

    def ffn(rows):
        gate_val = jnp.dot(rows, w_gate[0], preferred_element_type=jnp.float32)
        up_val = jnp.dot(rows, w_up[0], preferred_element_type=jnp.float32)
        inner = (jax.nn.silu(gate_val) * up_val).astype(jnp.bfloat16)
        return jnp.dot(inner, w_down[0], preferred_element_type=jnp.float32).astype(jnp.bfloat16)

    def layer(states):
        normed = rms_scale(states, layer_gain[0]).astype(jnp.bfloat16)
        packed = jnp.dot(pack, normed, preferred_element_type=jnp.float32).astype(jnp.bfloat16)
        mine = exchange(packed)
        other = swap_core(mine)
        logits = jnp.dot(normed, router[0], preferred_element_type=jnp.float32)
        affinity = jax.nn.sigmoid(jnp.sum(jnp.where(chosen, logits[:, None, :], 0.0), -1))
        weight = affinity / jnp.sum(affinity, -1, keepdims=True)
        mix = jnp.sum(jnp.where(hit, 2.5 * weight[:, :, None], 0.0), 1)
        mix_hi = lax.reduce_precision(mix, 8, 7)
        mix_lo = (mix - mix_hi).astype(jnp.bfloat16)
        mix_hi = mix_hi.astype(jnp.bfloat16)
        parts = ffn(jnp.concatenate([mine, other], 0))
        half = parts.shape[0] // 2
        total = parts[:half].astype(jnp.float32) + swap_core(parts[half:]).astype(jnp.float32)
        back = exchange(total.astype(jnp.bfloat16))
        mixed = jnp.dot(mix_hi, back, preferred_element_type=jnp.float32)
        mixed = mixed + jnp.dot(mix_lo, back, preferred_element_type=jnp.float32)
        return (states.astype(jnp.float32) + mixed).astype(jnp.bfloat16)

    states = hidden_in.reshape(micro * toks, width)
    for tick in range(sections):
        states = layer(states)
        if tick < sections - 1:
            states = lax.ppermute(states, "section", [(tick, tick + 1)])

    states = states.reshape(micro, toks, width)
    last = sections - 1
    mine = states[last % micro]
    for s in range(sections - 1):
        moved = lax.ppermute(states[s % micro], "section", [(last, s)])
        mine = jnp.where(section_pos == s, moved, mine)
    final = rms_scale(mine, final_gain).astype(jnp.bfloat16)
    near = exchange(jnp.broadcast_to(final[None], (groups, toks, width)).reshape(groups * toks, width))
    rows = jnp.concatenate([near, swap_core(near)], 0)

    vocab = head.shape[0]
    my_targets = lax.dynamic_index_in_dim(targets, batch_pos, 0, keepdims=False)
    my_targets = my_targets.reshape(groups, PAIR, toks).transpose(1, 0, 2)
    my_targets = jnp.where(parity == 0, my_targets, my_targets[::-1]).reshape(-1)
    logits = [
        jnp.dot(rows, block.T, preferred_element_type=jnp.float32) for block in head_blocks
    ]
    peak = logits[0].max(-1)
    for block in logits[1:]:
        peak = jnp.maximum(peak, block.max(-1))
    summed = jnp.zeros_like(peak)
    target = jnp.zeros_like(peak)
    for shift, block in enumerate(logits):
        owner = section_pos - batch_pos + (batch_pos - shift) % micro
        start = (owner * members + member_pos) * vocab
        ids = start + jnp.arange(vocab, dtype=jnp.int32)
        summed = summed + jnp.sum(jnp.exp(block - peak[:, None]), -1)
        target = target + jnp.sum(jnp.where(my_targets[:, None] == ids[None, :], block, 0.0), -1)
    stats = jnp.stack([peak, summed, target]).reshape(3, PAIR, groups * toks)
    stats = jnp.where(parity == 0, stats, stats[:, ::-1]).reshape(1, 3 * PAIR * groups * toks)
    world = sections * members
    stats = lax.all_to_all(
        jnp.broadcast_to(stats, (world, stats.shape[1])),
        ("section", "expert"),
        split_axis=0,
        concat_axis=0,
        tiled=True,
    )
    stats = stats.reshape(sections // micro, micro, members, 3, PAIR, groups, toks)
    peaks, sums, hits = stats[:, :, :, 0], stats[:, :, :, 1], stats[:, :, :, 2]
    top = jnp.max(peaks, (0, 2), keepdims=True)
    total = jnp.sum(sums * jnp.exp(peaks - top), (0, 2))
    logprob = jnp.sum(hits, (0, 2)) - (top[0, :, 0] + jnp.log(total))
    logprob = logprob.transpose(0, 2, 1, 3).reshape(micro, members * toks)
    token_part = lax.dynamic_slice_in_dim(logprob, member_pos * toks, toks, 1)
    member = seq_ids[:, :, None] == jnp.arange(SEQS, dtype=jnp.int32)[None, None, :]
    sums = jnp.sum(jnp.where(member, logprob[..., None], 0.0), 1)
    counts = jnp.sum(member.astype(jnp.float32), 1)
    return (token_part, sums / counts)


def solution(mesh):
    return jax.shard_map(
        body,
        mesh=mesh,
        in_specs=(
            P(None, "expert", None),
            P("section", None),
            P("section", None, None),
            P("section", None, "expert"),
            P("section", None, "expert"),
            P("section", "expert", None),
            P(),
            P(("section", "expert"), None),
            P("section", None, "expert", None),
            P(),
            P(),
        ),
        out_specs=(P(None, "expert"), P()),
        check_vma=False,
    )
```

```python
import jax
import jax.numpy as jnp
from jax import lax
from jax.experimental import pallas as pl
from jax.experimental.pallas import tpu as pltpu
from jax.sharding import PartitionSpec as P


SEQS = 4
PAIR = 2
HALVES = 2
LANES = 128
MIB = 1024 * 1024
VMEM = pl.BlockSpec(memory_space=pltpu.VMEM)
HBM = pl.BlockSpec(memory_space=pltpu.HBM)
ANY = pl.BlockSpec(memory_space=pl.ANY)
F32 = jnp.float32
BF16 = jnp.bfloat16


def call(kernel, outs, ins, specs, scratch=(), flops=1, vmem=32, moved=None):
    if moved is None:
        moved = sum(a.size * a.dtype.itemsize for a in ins)
    ins = [
        pltpu.with_memory_space_constraint(a, pltpu.HBM) if spec is HBM else a
        for a, spec in zip(ins, specs)
    ]
    return pl.pallas_call(
        kernel,
        out_shape=tuple(jax.ShapeDtypeStruct(shape, dtype) for shape, dtype in outs),
        in_specs=specs,
        out_specs=tuple(VMEM for _ in outs),
        scratch_shapes=scratch,
        compiler_params=pltpu.CompilerParams(vmem_limit_bytes=vmem * MIB),
        cost_estimate=pl.CostEstimate(flops=flops, bytes_accessed=moved, transcendentals=0),
    )(*ins)


def iota(shape, dim):
    return lax.broadcasted_iota(jnp.int32, shape, dim)


def dot(a, b, contract=(1, 0)):
    dims = (((contract[0],), (contract[1],)), ((), ()))
    return lax.dot_general(a, b, dims, preferred_element_type=F32)


def places_of(routes, cap):
    toks = routes[0].shape[0]
    lane = iota((toks, LANES), 1)
    named = jnp.zeros((toks, LANES), F32)
    for route in routes:
        named = named + (lane == route).astype(F32)
    earlier = (iota((toks, toks), 1) < iota((toks, toks), 0)).astype(BF16)
    ahead = dot(earlier, named.astype(BF16))
    places = []
    for k, route in enumerate(routes):
        slot = jnp.sum(jnp.where(lane == route, ahead, 0.0), 1, keepdims=True).astype(jnp.int32)
        for other in routes[:k]:
            slot = slot + (other == route).astype(jnp.int32)
        places.append(route * cap + slot)
    return places


def columns(table, start, batches, tops, batch):
    out = []
    for k in range(tops):
        if isinstance(batch, int):
            col = start + batch * tops + k
            out.append(table[:, col : col + 1].astype(jnp.int32))
            continue
        taken = table[:, start + k : start + k + 1]
        for m in range(1, batches):
            col = start + m * tops + k
            taken = jnp.where(batch == m, table[:, col : col + 1], taken)
        out.append(taken.astype(jnp.int32))
    return out


def prep_kernel(dims, *refs):
    sources, head_hbm, refs = refs[:5], refs[5], refs[6:]
    packed_ref, small_ref, states_ref, early_ref = refs[:4]
    held, sems = refs[4:9], refs[9]
    hidden_ref, gain_ref, router_ref, route_ref, final_ref = held
    copies = [pltpu.make_async_copy(*pair, sems.at[i]) for i, pair in enumerate(zip(sources, held))]
    copy = pltpu.make_async_copy(head_hbm.at[pl.ds(0, early_ref.shape[0])], early_ref, sems.at[5])
    for each in copies + [copy]:
        each.start()
    for each in copies:
        each.wait()
    batches, toks, width, experts, splits, tops, cap = dims
    wide = width // HALVES
    batch = lax.axis_index("section") % batches
    count = packed_ref.shape[0]
    lane = iota((toks, count), 1)
    lane_place = lane // (splits * batches * cap) * cap + lane % cap
    lane_batch = lane // cap % batches
    picks, normed = [], []
    own = hidden_ref[0]
    eye = (iota((toks, toks), 0) == iota((toks, toks), 1)).astype(F32)
    table = jnp.concatenate(
        [dot(eye, route_ref[m].astype(F32), (1, 1)) for m in range(batches)]
        + [jnp.zeros((toks, LANES - batches * tops), F32)],
        1,
    )
    for m in range(batches):
        hidden = hidden_ref[m]
        values = hidden.astype(F32)
        factor = lax.rsqrt(jnp.mean(values * values, -1, keepdims=True) + 1e-06)
        normed.append((values * factor * gain_ref[...]).astype(BF16))
        hit = jnp.zeros((toks, count), F32)
        for place in places_of(columns(table, 0, batches, tops, m), cap):
            hit = hit + ((lane_place == place) & (lane_batch == m)).astype(F32)
        picks.append(hit.astype(BF16))
        if m:
            own = jnp.where(batch == m, hidden, own)
    packed = dot(jnp.concatenate(picks, 0), jnp.concatenate(normed, 0), (0, 0))
    packed_ref[...] = packed.astype(BF16)
    small_ref[...] = jnp.zeros_like(small_ref)
    small_ref[0:1, 0:width] = gain_ref[...]
    small_ref[1 : 1 + experts, 0:width] = router_ref[...].astype(F32)
    small_ref[1 + experts : 2 + experts, 0:width] = final_ref[...][None, :]
    small_ref[0:toks, width:] = table
    for half in range(HALVES):
        states_ref[half * toks : (half + 1) * toks, :] = own[:, half * wide : (half + 1) * wide]
    copy.wait()


def prep(dims, table_rows, early, hidden_in, layer_gain, router, routing, final_gain, head):
    batches, toks, width, experts, splits, _, cap = dims
    arrays = (
        hidden_in,
        layer_gain,
        router[0].T,
        routing[0].transpose(0, 2, 1),
        final_gain,
    )
    return call(
        lambda *refs: prep_kernel(dims, *refs),
        [
            ((experts * splits * batches * cap, width), BF16),
            ((table_rows, width + LANES), F32),
            ((HALVES * toks, width // HALVES), BF16),
            ((early, width), BF16),
        ],
        (*arrays, head),
        [HBM] * 6,
        [pltpu.VMEM(a.shape, a.dtype) for a in arrays] + [pltpu.SemaphoreType.DMA((6,))],
    )


def plan(dims, layer, states, shifted, sections):
    batches, toks, width, experts, splits, tops, cap = dims
    wide = width // HALVES
    section = lax.axis_index("section")
    table = pick_layer(shifted, section, layer, sections)
    routes = columns(table[:toks, width:], 0, batches, tops, section % batches)
    places = places_of(routes, cap)
    values = [states[h * toks : (h + 1) * toks].astype(F32) for h in range(HALVES)]
    square = sum(jnp.sum(v * v, -1, keepdims=True) for v in values)
    factor = lax.rsqrt(square / width + 1e-06)
    logits = 0.0
    for half in range(HALVES):
        cols = slice(half * wide, (half + 1) * wide)
        normed = (values[half] * factor * table[0:1, cols]).astype(BF16)
        logits = logits + dot(normed, table[:, cols].astype(BF16), (1, 1))
    lane = iota(logits.shape, 1)
    scores = [
        jax.nn.sigmoid(jnp.sum(jnp.where(lane == route + 1, logits, 0.0), 1, keepdims=True))
        for route in routes
    ]
    whole = sum(scores)
    count = experts * splits * HALVES * cap
    row = iota((toks, count), 1)
    row_place = row // (splits * HALVES * cap) * cap + row % cap
    row_half = row // cap % HALVES
    mix = jnp.zeros((toks, count), F32)
    for score, place in zip(scores, places):
        mix = mix + jnp.where(row_place == place, 2.5 * (score / whole), 0.0)
    return [jnp.where(row_half == half, mix, 0.0) for half in range(HALVES)]


def pick_layer(shifted, section, layer, sections):
    shift = (section - layer + sections) % sections
    table = shifted[0]
    for k in range(1, sections):
        table = jnp.where(shift == k, shifted[k], table)
    return table


def next_pack(dims, layer, shifted, sections, pack_ref, gain_ref):
    batches, toks, width, experts, splits, tops, cap = dims
    wide = width // HALVES
    section = lax.axis_index("section")
    table = pick_layer(shifted, section, layer, sections)
    routes = columns(table[:toks, width:], 0, batches, tops, section % batches)
    count = pack_ref.shape[1]
    row = iota((toks, count), 1)
    row_place = row // (splits * HALVES * cap) % experts * cap + row % cap
    row_half = row // cap % HALVES
    hit = jnp.zeros((toks, count), F32)
    for place in places_of(routes, cap):
        hit = hit + (row_place == place).astype(F32)
    for half in range(HALVES):
        flags = jnp.where(row_half == half, hit, 0.0)
        pack_ref[half * toks : (half + 1) * toks, :] = flags.astype(BF16)
        gain_ref[half : half + 1, :] = table[0:1, half * wide : (half + 1) * wide]


def ffn_kernel(dims, layer, sections, chunks, *refs):
    batches, toks, width, experts, _, _, cap = dims
    last = layer == sections - 1
    near_ref, far_ref, gate_hbm, up_hbm, down_hbm, head_hbm, states_ref = refs[:7]
    shifted_refs, refs = refs[7 : 7 + sections], refs[7 + sections :]
    keep_ref, send_ref, mix_ref = refs[:3]
    refs = refs[3:]
    gain_ref, extra_ref, refs = refs[0], refs[1], refs[2:]
    gate_ref, up_ref, down_ref, sems = refs
    split = layer > 0
    count, wide = keep_ref.shape
    rows = count // HALVES
    groups = rows // (batches * cap)
    depth = width // chunks

    copies = []
    for c in range(chunks):
        part = pl.ds(c * depth, depth)
        copies.append(pltpu.make_async_copy(gate_hbm.at[part], gate_ref.at[part], sems.at[2 * c]))
        copies.append(pltpu.make_async_copy(up_hbm.at[part], up_ref.at[part], sems.at[2 * c + 1]))
    for half in range(HALVES):
        part = pl.ds(half * wide, wide)
        copies.append(
            pltpu.make_async_copy(down_hbm.at[:, part], down_ref.at[:, part], sems.at[2 * chunks + half])
        )
    if last:
        late = extra_ref.shape[0]
        rest = pl.ds(head_hbm.shape[0] - late, late)
        copies.append(pltpu.make_async_copy(head_hbm.at[rest], extra_ref, sems.at[2 * chunks + HALVES]))
    for copy in copies:
        copy.start()

    shifted = [ref[...] for ref in shifted_refs]
    for half, mix in enumerate(plan(dims, layer, states_ref[...], shifted, sections)):
        high = mix.astype(BF16)
        mix_ref[half * toks : (half + 1) * toks, :] = high
        low = (mix - high.astype(F32)).astype(BF16)
        mix_ref[(HALVES + half) * toks : (HALVES + half + 1) * toks, :] = low
    if last:
        for half in range(HALVES):
            cols = slice(half * wide, (half + 1) * wide)
            gain_ref[half : half + 1, :] = shifted[0][1 + experts : 2 + experts, cols]
    else:
        next_pack(dims, layer + 1, shifted, sections, extra_ref, gain_ref)

    def whole(ref):
        if not split:
            return ref[...]
        row, col = iota((rows, count), 0), iota((rows, count), 1)
        parts = []
        for half in range(HALVES):
            pick = row // cap * (HALVES * cap) + half * cap + row % cap == col
            parts.append(dot(pick.astype(BF16), ref[...]).astype(BF16))
        return jnp.concatenate(parts, 1)

    row, col = iota((count, rows), 0), iota((count, rows), 1)
    slot, block, side = row % cap, row // (HALVES * cap), row // cap % HALVES
    if split:
        source = block * cap + slot
    else:
        source = (block % groups * batches + block // groups) * cap + slot

    data = jnp.concatenate([whole(near_ref), whole(far_ref)], 0)
    gate_val = up_val = 0.0
    for c in range(chunks):
        copies[2 * c].wait()
        copies[2 * c + 1].wait()
        part = slice(c * depth, (c + 1) * depth)
        gate_val = gate_val + dot(data[:, part], gate_ref[part, :])
        up_val = up_val + dot(data[:, part], up_ref[part, :])
    inner = (gate_val / (1.0 + jnp.exp(-gate_val)) * up_val).astype(BF16)
    keep = send = 0.0
    for half in range(HALVES):
        copies[2 * chunks + half].wait()
        part = dot(inner, down_ref[:, half * wide : (half + 1) * wide]).astype(BF16)
        pick = ((source == col) & (side == half)).astype(BF16)
        send = send + dot(pick, part[rows:])
        keep = keep + dot(pick, part[:rows])
    send_ref[...] = send.astype(BF16)
    keep_ref[...] = keep.astype(BF16)
    for copy in copies[2 * chunks + HALVES :]:
        copy.wait()


def ffn(dims, layer, sections, near, far, gate, up, down, head, early, states, shifted):
    batches, toks, width, experts, splits, _, cap = dims
    hidden = gate.shape[1]
    wide = width // HALVES
    back = experts * splits * HALVES * cap
    count = batches * back
    chunks = 4
    outs = [((count, wide), BF16), ((count, wide), BF16), ((2 * HALVES * toks, back), BF16)]
    outs.append(((HALVES, wide), F32))
    if layer < sections - 1:
        outs.append(((HALVES * toks, sections * back), BF16))
    else:
        outs.append(((head.shape[0] - early, width), BF16))
    ins = (near, far, gate, up, down, head, states, *shifted)
    specs = [VMEM, VMEM, HBM, HBM, HBM, HBM] + [VMEM] * (1 + sections)
    scratch = [
        pltpu.VMEM((width, hidden), BF16),
        pltpu.VMEM((width, hidden), BF16),
        pltpu.VMEM((hidden, width), BF16),
        pltpu.SemaphoreType.DMA((2 * chunks + HALVES + 1,)),
    ]
    return call(
        lambda *refs: ffn_kernel(dims, layer, sections, chunks, *refs),
        outs,
        ins,
        specs,
        scratch,
        flops=6 * count * width * hidden,
    )


def head_kernel(batches, early, near_ref, far_ref, target_ref, *refs):
    others = batches - 1
    sources, refs = refs[: 1 + 2 * others], refs[1 + 2 * others :]
    out_ref, table_ref, sems = refs
    vocab = sources[0].shape[0]
    section, member = lax.axis_index("section"), lax.axis_index("expert")
    members = lax.axis_size("expert")
    batch = section % batches
    copies, spot = [], 0
    for i, source in enumerate(sources):
        size = source.shape[0]
        copies.append(pltpu.make_async_copy(source, table_ref.at[pl.ds(spot, size)], sems.at[i]))
        spot += size
    for copy in copies:
        copy.start()

    toks = near_ref.shape[0] + far_ref.shape[0]
    each = toks // members
    col = iota((toks, toks), 1)
    core = (col // (toks // PAIR) + member) % PAIR
    moved = iota((toks, toks), 0) == (col // each % (members // PAIR) * PAIR + core) * each + col % each
    moved = moved.astype(F32)
    ids = target_ref[...].astype(F32)
    target = ids[0:1]
    for m in range(1, batches):
        target = jnp.where(batch == m, ids[m : m + 1], target)
    exact = lax.Precision.HIGHEST
    target = jnp.broadcast_to(target, (8, toks))
    target = jnp.dot(target, moved, precision=exact, preferred_element_type=F32)[0:1].astype(jnp.int32)

    rows = jnp.concatenate([near_ref[...], far_ref[...]], 0)
    for copy in copies[1:]:
        copy.wait()
    after = dot(table_ref[vocab:, :], rows, (1, 1))
    copies[0].wait()
    blocks, spot = [(dot(table_ref[:vocab, :], rows, (1, 1)), (section * members + member) * vocab)], 0
    for i, source in enumerate(sources[1:]):
        size = source.shape[0]
        shift = i % others + 1
        owner = section - batch + (batch - shift + batches) % batches
        start = (owner * members + member) * vocab + (early if i >= others else 0)
        blocks.append((after[spot : spot + size], start))
        spot += size
    peak = blocks[0][0].max(0, keepdims=True)
    for block, _ in blocks[1:]:
        peak = jnp.maximum(peak, block.max(0, keepdims=True))
    total = hit = 0.0
    for block, start in blocks:
        total = total + jnp.sum(jnp.exp(block - peak), 0, keepdims=True)
        hit = hit + jnp.sum(jnp.where(iota(block.shape, 0) + start == target, block, 0.0), 0, keepdims=True)
    both = jnp.concatenate([peak + jnp.log(total), hit, jnp.zeros((6, toks), F32)], 0)
    both = lax.dot_general(
        both, moved, (((1,), (1,)), ((), ())), precision=exact, preferred_element_type=F32
    )
    out = jnp.concatenate([both[0:1], both[1:2]], 1)
    out_ref[...] = jnp.broadcast_to(out[None], out_ref.shape)


def final_kernel(batches, toks, stats_ref, seq_ref, token_ref, mean_ref):
    member = lax.axis_index("expert")
    members = lax.axis_size("expert")
    sections = lax.axis_size("section")
    count = members * toks
    stats = stats_ref[:, 0, :]
    spot = member * toks
    lane = iota((1, count), 1)
    seat = iota((1, SEQS), 1)
    for m in range(batches):
        rows = [stats[s * members : (s + 1) * members] for s in range(m, sections, batches)]
        rows = rows[0] if len(rows) == 1 else jnp.concatenate(rows, 0)
        local, hits = rows[:, :count], rows[:, count:]
        peak = jnp.max(local, 0, keepdims=True)
        lse = peak + jnp.log(jnp.sum(jnp.exp(local - peak), 0, keepdims=True))
        logprob = jnp.sum(hits, 0, keepdims=True) - lse
        ids = seq_ref[m : m + 1, :]
        means = jnp.zeros((1, SEQS), F32)
        for s in range(SEQS):
            inside = ids == s
            summed = jnp.sum(jnp.where(inside, logprob, 0.0), 1, keepdims=True)
            size = jnp.sum(jnp.where(inside, 1.0, 0.0), 1, keepdims=True)
            means = jnp.where(seat == s, summed / size, means)
        mean_ref[m : m + 1, :] = means
        mine = pltpu.roll(logprob, count - spot, 1)
        token_ref[m : m + 1, :] = mine[:, :toks]


def body(
    hidden_in, layer_gain, router, w_gate, w_up, w_down, final_gain, head, routing, targets, seq_ids
):
    batches, toks, width = hidden_in.shape
    experts = router.shape[2]
    tops = routing.shape[3]
    sections = lax.axis_size("section")
    members = lax.axis_size("expert")
    splits = members // experts // PAIR
    groups = members // PAIR
    cap = min(toks, 9 * toks * tops // (8 * experts))
    wide = width // HALVES
    dims = (batches, toks, width, experts, splits, tops, cap)
    same_core = [[g * PAIR + c for g in range(groups)] for c in range(PAIR)]
    same_core_all = [
        [s * members + g * PAIR + c for s in range(sections) for g in range(groups)]
        for c in range(PAIR)
    ]
    partner = [(i, i ^ 1) for i in range(members)]

    def exchange(rows):
        return lax.all_to_all(
            rows, "expert", split_axis=0, concat_axis=0, axis_index_groups=same_core, tiled=True
        )

    def exchange_all(rows):
        return lax.all_to_all(
            rows,
            ("section", "expert"),
            split_axis=0,
            concat_axis=0,
            axis_index_groups=same_core_all,
            tiled=True,
        )

    def swap_core(rows):
        return lax.ppermute(rows, "expert", partner)

    def by_section(array, shift, across):
        return lax.ppermute(
            array,
            "section",
            [(s, s - s % across + (s + shift) % across) for s in range(sections)],
        )

    early = head.shape[0] * 5 // 8 // 16 * 16
    table_rows = max(-(-(2 + experts) // 8) * 8, toks)
    packed, small, states, early_head = prep(
        dims, table_rows, early, hidden_in, layer_gain, router, routing, final_gain, head
    )
    first_parts = []
    for shift in range(1, batches):
        first_parts.append(by_section(early_head, shift, batches))
    near = exchange(packed)

    shifted = [small]
    for shift in range(1, sections):
        shifted.append(by_section(small, shift, sections))

    size = groups * HALVES * cap
    for tick in range(sections):
        far = swap_core(near)
        keep, send, mixes, gain, extra = ffn(
            dims,
            tick,
            sections,
            near,
            far,
            w_gate[0],
            w_up[0],
            w_down[0],
            head,
            early,
            states,
            shifted,
        )
        total = (keep.astype(F32) + swap_core(send).astype(F32)).astype(BF16)
        if sections > batches:
            total = jnp.concatenate([total] * (sections // batches), 0)
        back = exchange_all(total)[tick * size : (tick + 1) * size]
        mixed = dot(mixes, back)
        states = states.astype(F32) + mixed[: HALVES * toks] + mixed[HALVES * toks :]
        states = states.astype(BF16)
        values = states.astype(F32).reshape(HALVES, toks, wide)
        factor = lax.rsqrt(jnp.sum(values * values, (0, 2), keepdims=True) / width + 1e-06)
        if tick == sections - 1:
            break
        normed = (values * factor * gain[:, None, :]).astype(BF16)
        packed = dot(extra, normed.reshape(HALVES * toks, wide), (0, 0)).astype(BF16)
        near = exchange_all(packed)
        if sections > batches:
            base = tick + 1 - (tick + 1) % batches
            near = near[base * size : (base + batches) * size]

    states, late_head = lax.optimization_barrier((states, extra))
    late_parts = []
    for shift in range(1, batches):
        late_parts.append(by_section(late_head, shift, batches))
    final = (values * factor * gain[:, None, :]).astype(BF16)
    final = jnp.concatenate([final[h] for h in range(HALVES)], 1)
    near = exchange(jnp.broadcast_to(final[None], (groups, toks, width)).reshape(groups * toks, width))
    far = swap_core(near)
    world = sections * members
    (stats,) = call(
        lambda *refs: head_kernel(batches, early, *refs),
        [((world, 1, 2 * members * toks), F32)],
        (near, far, targets, head, *first_parts, *late_parts),
        [VMEM] * 3 + [HBM] + [ANY] * (2 * batches - 2),
        [
            pltpu.VMEM((batches * head.shape[0], width), BF16),
            pltpu.SemaphoreType.DMA((2 * batches - 1,)),
        ],
        flops=4 * head.size * members * toks,
    )
    stats = lax.all_to_all(stats, ("section", "expert"), split_axis=0, concat_axis=0, tiled=True)
    return call(
        lambda *refs: final_kernel(batches, toks, *refs),
        [((batches, toks), F32), ((batches, SEQS), F32)],
        (stats, seq_ids),
        [VMEM] * 2,
    )


def solution(mesh):
    return jax.shard_map(
        body,
        mesh=mesh,
        in_specs=(
            P(None, "expert", None),
            P("section", None),
            P("section", None, None),
            P("section", None, "expert"),
            P("section", None, "expert"),
            P("section", "expert", None),
            P(),
            P(("section", "expert"), None),
            P("section", None, "expert", None),
            P(),
            P(),
        ),
        out_specs=(P(None, "expert"), P()),
        check_vma=False,
    )
```

```python
import jax
import jax.numpy as jnp
from jax import lax
from jax.experimental import pallas as pl
from jax.experimental.pallas import tpu as pltpu
from jax.sharding import PartitionSpec as P


SEQS = 4
PAIR = 2
HALVES = 2
LANES = 128
MIB = 1024 * 1024
VMEM = pl.BlockSpec(memory_space=pltpu.VMEM)
HBM = pl.BlockSpec(memory_space=pltpu.HBM)
ANY = pl.BlockSpec(memory_space=pl.ANY)
F32 = jnp.float32
BF16 = jnp.bfloat16


def call(kernel, outs, ins, specs, scratch=(), flops=1, vmem=32, moved=None):
    if moved is None:
        moved = sum(a.size * a.dtype.itemsize for a in ins)
    ins = [
        pltpu.with_memory_space_constraint(a, pltpu.HBM) if spec is HBM else a
        for a, spec in zip(ins, specs)
    ]
    return pl.pallas_call(
        kernel,
        out_shape=tuple(
            pltpu.VMEM(*out[:2]) if out[2:] else jax.ShapeDtypeStruct(*out) for out in outs
        ),
        in_specs=specs,
        out_specs=tuple(VMEM for _ in outs),
        scratch_shapes=scratch,
        compiler_params=pltpu.CompilerParams(vmem_limit_bytes=vmem * MIB),
        cost_estimate=pl.CostEstimate(flops=flops, bytes_accessed=moved, transcendentals=0),
    )(*ins)


def iota(shape, dim):
    return lax.broadcasted_iota(jnp.int32, shape, dim)


def dot(a, b, contract=(1, 0)):
    dims = (((contract[0],), (contract[1],)), ((), ()))
    return lax.dot_general(a, b, dims, preferred_element_type=F32)


def places_of(routes, cap):
    toks = routes[0].shape[0]
    lane = iota((toks, LANES), 1)
    named = jnp.zeros((toks, LANES), F32)
    for route in routes:
        named = named + (lane == route).astype(F32)
    earlier = (iota((toks, toks), 1) < iota((toks, toks), 0)).astype(BF16)
    ahead = dot(earlier, named.astype(BF16))
    places = []
    for k, route in enumerate(routes):
        slot = jnp.sum(jnp.where(lane == route, ahead, 0.0), 1, keepdims=True).astype(jnp.int32)
        for other in routes[:k]:
            slot = slot + (other == route).astype(jnp.int32)
        places.append(route * cap + slot)
    return places


def columns(table, start, batches, tops, batch):
    out = []
    for k in range(tops):
        if isinstance(batch, int):
            col = start + batch * tops + k
            out.append(table[:, col : col + 1].astype(jnp.int32))
            continue
        taken = table[:, start + k : start + k + 1]
        for m in range(1, batches):
            col = start + m * tops + k
            taken = jnp.where(batch == m, table[:, col : col + 1], taken)
        out.append(taken.astype(jnp.int32))
    return out


def prep_kernel(dims, *refs):
    sources, head_hbm, refs = refs[:5], refs[5], refs[6:]
    packed_ref, small_ref, states_ref, early_ref = refs[:4]
    held, sems = refs[4:9], refs[9]
    hidden_ref, gain_ref, router_ref, route_ref, final_ref = held
    copies = [pltpu.make_async_copy(*pair, sems.at[i]) for i, pair in enumerate(zip(sources, held))]
    copy = pltpu.make_async_copy(head_hbm.at[pl.ds(0, early_ref.shape[0])], early_ref, sems.at[5])
    for each in copies + [copy]:
        each.start()
    for each in copies:
        each.wait()
    batches, toks, width, experts, _, tops, cap = dims
    wide = width // HALVES
    batch = lax.axis_index("section") % batches
    count = packed_ref.shape[0]
    lane = iota((toks, count), 1)
    lane_place = lane // (batches * cap) * cap + lane % cap
    lane_batch = lane // cap % batches
    picks, normed = [], []
    own = hidden_ref[0]
    eye = (iota((toks, toks), 0) == iota((toks, toks), 1)).astype(F32)
    table = jnp.concatenate(
        [dot(eye, route_ref[m].astype(F32), (1, 1)) for m in range(batches)]
        + [jnp.zeros((toks, LANES - batches * tops), F32)],
        1,
    )
    for m in range(batches):
        hidden = hidden_ref[m]
        values = hidden.astype(F32)
        factor = lax.rsqrt(jnp.mean(values * values, -1, keepdims=True) + 1e-06)
        normed.append((values * factor * gain_ref[...]).astype(BF16))
        hit = jnp.zeros((toks, count), F32)
        for place in places_of(columns(table, 0, batches, tops, m), cap):
            hit = hit + ((lane_place == place) & (lane_batch == m)).astype(F32)
        picks.append(hit.astype(BF16))
        if m:
            own = jnp.where(batch == m, hidden, own)
    packed = dot(jnp.concatenate(picks, 0), jnp.concatenate(normed, 0), (0, 0))
    packed_ref[...] = packed.astype(BF16)
    small_ref[...] = jnp.zeros_like(small_ref)
    small_ref[0:1, 0:width] = gain_ref[...]
    small_ref[1 : 1 + experts, 0:width] = router_ref[...].astype(F32)
    small_ref[1 + experts : 2 + experts, 0:width] = final_ref[...][None, :]
    small_ref[0:toks, width:] = table
    for half in range(HALVES):
        states_ref[half * toks : (half + 1) * toks, :] = own[:, half * wide : (half + 1) * wide]
    copy.wait()


def prep(dims, table_rows, early, hidden_in, layer_gain, router, routing, final_gain, head):
    batches, toks, width, experts, _, _, cap = dims
    arrays = (
        hidden_in,
        layer_gain,
        router[0].T,
        routing[0].transpose(0, 2, 1),
        final_gain,
    )
    return call(
        lambda *refs: prep_kernel(dims, *refs),
        [
            ((experts * batches * cap, width), BF16),
            ((table_rows, width + LANES), F32),
            ((HALVES * toks, width // HALVES), BF16),
            ((early, width), BF16),
        ],
        (*arrays, head),
        [HBM] * 6,
        [pltpu.VMEM(a.shape, a.dtype) for a in arrays] + [pltpu.SemaphoreType.DMA((6,))],
    )


def plan(dims, layer, states, shifted, sections):
    batches, toks, width, experts, splits, tops, cap = dims
    wide = width // HALVES
    section = lax.axis_index("section")
    table = pick_layer(shifted, section, layer, sections)
    routes = columns(table[:toks, width:], 0, batches, tops, section % batches)
    places = places_of(routes, cap)
    values = [states[h * toks : (h + 1) * toks].astype(F32) for h in range(HALVES)]
    square = sum(jnp.sum(v * v, -1, keepdims=True) for v in values)
    factor = lax.rsqrt(square / width + 1e-06)
    logits = 0.0
    for half in range(HALVES):
        cols = slice(half * wide, (half + 1) * wide)
        normed = (values[half] * factor * table[0:1, cols]).astype(BF16)
        logits = logits + dot(normed, table[:, cols].astype(BF16), (1, 1))
    lane = iota(logits.shape, 1)
    scores = [
        jax.nn.sigmoid(jnp.sum(jnp.where(lane == route + 1, logits, 0.0), 1, keepdims=True))
        for route in routes
    ]
    whole = sum(scores)
    count = experts * splits * HALVES * cap
    row = iota((toks, count), 1)
    row_place = row // (splits * HALVES * cap) * cap + row % cap
    row_half = row // cap % HALVES
    mix = jnp.zeros((toks, count), F32)
    for score, place in zip(scores, places):
        mix = mix + jnp.where(row_place == place, 2.5 * (score / whole), 0.0)
    return [jnp.where(row_half == half, mix, 0.0) for half in range(HALVES)]


def pick_layer(shifted, section, layer, sections):
    shift = (section - layer + sections) % sections
    table = shifted[0]
    for k in range(1, sections):
        table = jnp.where(shift == k, shifted[k], table)
    return table


def next_pack(dims, layer, shifted, sections, pack_ref, gain_ref):
    batches, toks, width, experts, _, tops, cap = dims
    wide = width // HALVES
    section = lax.axis_index("section")
    table = pick_layer(shifted, section, layer, sections)
    routes = columns(table[:toks, width:], 0, batches, tops, section % batches)
    count = pack_ref.shape[1]
    row = iota((toks, count), 1)
    row_place = row // (HALVES * cap) % experts * cap + row % cap
    row_half = row // cap % HALVES
    hit = jnp.zeros((toks, count), F32)
    for place in places_of(routes, cap):
        hit = hit + (row_place == place).astype(F32)
    for half in range(HALVES):
        flags = jnp.where(row_half == half, hit, 0.0)
        pack_ref[half * toks : (half + 1) * toks, :] = flags.astype(BF16)
        gain_ref[half : half + 1, :] = table[0:1, half * wide : (half + 1) * wide]


def ready_kernel(dims, layer, sections, *refs):
    _, toks, width, experts, _, _, _ = dims
    last = layer == sections - 1
    wide = width // HALVES
    weights, head_hbm, states_ref = refs[:3], refs[3], refs[4]
    shifted_refs, refs = refs[5 : 5 + sections], refs[5 + sections :]
    mix_ref, gain_ref, refs = refs[0], refs[1], refs[2:]
    if not last:
        pack_ref, refs = refs[0], refs[1:]
    held, sems = refs[:3], refs[-1]
    copies = [pltpu.make_async_copy(*pair, sems.at[i]) for i, pair in enumerate(zip(weights, held))]
    if layer == 0:
        late = refs[3].shape[0]
        rest = pl.ds(head_hbm.shape[0] - late, late)
        copies.append(pltpu.make_async_copy(head_hbm.at[rest], refs[3], sems.at[len(weights)]))
    for copy in copies:
        copy.start()

    shifted = [ref[...] for ref in shifted_refs]
    for half, mix in enumerate(plan(dims, layer, states_ref[...], shifted, sections)):
        high = mix.astype(BF16)
        mix_ref[half * toks : (half + 1) * toks, :] = high
        low = (mix - high.astype(F32)).astype(BF16)
        mix_ref[(HALVES + half) * toks : (HALVES + half + 1) * toks, :] = low
    if last:
        for half in range(HALVES):
            cols = slice(half * wide, (half + 1) * wide)
            gain_ref[half : half + 1, :] = shifted[0][1 + experts : 2 + experts, cols]
    else:
        next_pack(dims, layer + 1, shifted, sections, pack_ref, gain_ref)

    for copy in copies:
        copy.wait()


def ready(dims, layer, sections, weights, head, early, states, shifted):
    _, toks, width, experts, splits, _, cap = dims
    back = experts * splits * HALVES * cap
    outs = [((2 * HALVES * toks, back), BF16), ((HALVES, width // HALVES), F32)]
    if layer < sections - 1:
        outs.append(((HALVES * toks, sections * experts * HALVES * cap), BF16))
    outs += [(weight.shape, BF16, True) for weight in weights]
    if layer == 0:
        outs.append(((head.shape[0] - early, width), BF16))
    return call(
        lambda *refs: ready_kernel(dims, layer, sections, *refs),
        outs,
        (*weights, head, states, *shifted),
        [HBM] * 4 + [VMEM] * (1 + sections),
        [pltpu.SemaphoreType.DMA((4,))],
    )


def expert_kernel(dims, split, *refs):
    batches, _, _, experts, splits, _, cap = dims
    sources, refs = refs[: PAIR * splits], refs[PAIR * splits :]
    gate_ref, up_ref, down_ref, keep_ref, send_ref = refs
    count, wide = keep_ref.shape
    rows = count // HALVES
    each = rows // splits
    place = lax.axis_index("expert") // PAIR % splits

    def whole(ref):
        if not split:
            return ref[...]
        shape = (each, HALVES * each)
        row, col = iota(shape, 0), iota(shape, 1)
        parts = []
        for half in range(HALVES):
            pick = row // cap * (HALVES * cap) + half * cap + row % cap == col
            parts.append(dot(pick.astype(BF16), ref[...]).astype(BF16))
        return jnp.concatenate(parts, 1)

    row, col = iota((count, rows), 0), iota((count, rows), 1)
    slot, side = row % cap, row // cap % HALVES
    shift = (place - row // (HALVES * cap) % splits + splits) % splits
    block = row // (HALVES * cap * splits)
    if not split:
        block = block % experts * batches + block // experts
    source = shift * each + block * cap + slot
    data = jnp.concatenate([whole(ref) for ref in sources], 0)
    gate_val, up_val = dot(data, gate_ref[...]), dot(data, up_ref[...])
    inner = (gate_val / (1.0 + jnp.exp(-gate_val)) * up_val).astype(BF16)
    keep = send = 0.0
    for half in range(HALVES):
        part = dot(inner, down_ref[:, half * wide : (half + 1) * wide]).astype(BF16)
        pick = ((source == col) & (side == half)).astype(BF16)
        send = send + dot(pick, part[rows:])
        keep = keep + dot(pick, part[:rows])
    send_ref[...] = send.astype(BF16)
    keep_ref[...] = keep.astype(BF16)


def expert_rows(dims, layer, sources, weights):
    batches, _, width, experts, splits, _, cap = dims
    count = batches * experts * splits * HALVES * cap
    return call(
        lambda *refs: expert_kernel(dims, layer > 0, *refs),
        [((count, width // HALVES), BF16)] * 2,
        (*sources, *weights),
        [VMEM] * (len(sources) + 3),
        flops=6 * count * width * weights[0].shape[1],
    )


def advance_kernel(dims, layer, last, back_ref, mix_ref, states_ref, gain_ref, *refs):
    _, toks, width, _, _, _, _ = dims
    wide = width // HALVES
    size = mix_ref.shape[1]
    mixed = dot(mix_ref[...], back_ref[layer * size : (layer + 1) * size, :])
    states = states_ref[...].astype(F32) + mixed[: HALVES * toks] + mixed[HALVES * toks :]
    states = states.astype(BF16)
    values = states.astype(F32)
    square = jnp.sum(values * values, -1, keepdims=True)
    factor = lax.rsqrt(sum(square[h * toks : (h + 1) * toks] for h in range(HALVES)) / width + 1e-06)
    normed = [
        (values[h * toks : (h + 1) * toks] * factor * gain_ref[h : h + 1, :]).astype(BF16)
        for h in range(HALVES)
    ]
    if last:
        out_ref = refs[0]
        for h in range(HALVES):
            for copy in range(out_ref.shape[0] // toks):
                out_ref[copy * toks : (copy + 1) * toks, h * wide : (h + 1) * wide] = normed[h]
        return
    pack_ref, out_ref, packed_ref = refs
    out_ref[...] = states
    packed_ref[...] = dot(pack_ref[...], jnp.concatenate(normed, 0), (0, 0)).astype(BF16)


def advance(dims, layer, back, mixes, states, gain, pack):
    _, toks, width, experts, splits, _, _ = dims
    last = pack is None
    if last:
        outs = [((experts * splits * toks, width), BF16)]
    else:
        outs = [(states.shape, BF16), ((pack.shape[1], width // HALVES), BF16)]
    ins = (back, mixes, states, gain) + (() if last else (pack,))
    return call(
        lambda *refs: advance_kernel(dims, layer, last, *refs), outs, ins, [VMEM] * len(ins)
    )


def table_kernel(*refs):
    sources, table_ref, sems = refs[:-2], refs[-2], refs[-1]
    copies, spot = [], 0
    for i, source in enumerate(sources):
        size = source.shape[0]
        copies.append(pltpu.make_async_copy(source, table_ref.at[pl.ds(spot, size)], sems.at[i]))
        spot += size
    for copy in copies:
        copy.start()
    for copy in copies:
        copy.wait()


def head_kernel(batches, early, near_ref, far_ref, target_ref, table_ref, out_ref):
    others = batches - 1
    vocab = table_ref.shape[0] // batches
    section, member = lax.axis_index("section"), lax.axis_index("expert")
    members = lax.axis_size("expert")
    batch = section % batches
    toks = near_ref.shape[0] + far_ref.shape[0]
    each = toks // members
    col = iota((toks, toks), 1)
    core = (col // (toks // PAIR) + member) % PAIR
    moved = iota((toks, toks), 0) == (col // each % (members // PAIR) * PAIR + core) * each + col % each
    moved = moved.astype(F32)
    ids = target_ref[...].astype(F32)
    target = ids[0:1]
    for m in range(1, batches):
        target = jnp.where(batch == m, ids[m : m + 1], target)
    exact = lax.Precision.HIGHEST
    target = jnp.broadcast_to(target, (8, toks))
    target = jnp.dot(target, moved, precision=exact, preferred_element_type=F32)[0:1].astype(jnp.int32)

    rows = jnp.concatenate([near_ref[...], far_ref[...]], 0)
    logits = dot(table_ref[...], rows, (1, 1))
    blocks, spot = [(logits[:vocab], (section * members + member) * vocab)], vocab
    for i in range(2 * others):
        size = early if i < others else vocab - early
        owner = section - batch + (batch - i % others - 1 + batches) % batches
        start = (owner * members + member) * vocab + (early if i >= others else 0)
        blocks.append((logits[spot : spot + size], start))
        spot += size
    peak = blocks[0][0].max(0, keepdims=True)
    for block, _ in blocks[1:]:
        peak = jnp.maximum(peak, block.max(0, keepdims=True))
    total = hit = 0.0
    for block, start in blocks:
        total = total + jnp.sum(jnp.exp(block - peak), 0, keepdims=True)
        hit = hit + jnp.sum(jnp.where(iota(block.shape, 0) + start == target, block, 0.0), 0, keepdims=True)
    both = jnp.concatenate([peak + jnp.log(total), hit, jnp.zeros((6, toks), F32)], 0)
    both = lax.dot_general(
        both, moved, (((1,), (1,)), ((), ())), precision=exact, preferred_element_type=F32
    )
    out = jnp.concatenate([both[0:1], both[1:2]], 1)
    out_ref[...] = jnp.broadcast_to(out[None], out_ref.shape)


def final_kernel(batches, toks, stats_ref, seq_ref, token_ref, mean_ref):
    member = lax.axis_index("expert")
    members = lax.axis_size("expert")
    sections = lax.axis_size("section")
    count = members * toks
    stats = stats_ref[:, 0, :]
    spot = member * toks
    lane = iota((1, count), 1)
    seat = iota((1, SEQS), 1)
    for m in range(batches):
        rows = [stats[s * members : (s + 1) * members] for s in range(m, sections, batches)]
        rows = rows[0] if len(rows) == 1 else jnp.concatenate(rows, 0)
        local, hits = rows[:, :count], rows[:, count:]
        peak = jnp.max(local, 0, keepdims=True)
        lse = peak + jnp.log(jnp.sum(jnp.exp(local - peak), 0, keepdims=True))
        logprob = jnp.sum(hits, 0, keepdims=True) - lse
        ids = seq_ref[m : m + 1, :]
        means = jnp.zeros((1, SEQS), F32)
        for s in range(SEQS):
            inside = ids == s
            summed = jnp.sum(jnp.where(inside, logprob, 0.0), 1, keepdims=True)
            size = jnp.sum(jnp.where(inside, 1.0, 0.0), 1, keepdims=True)
            means = jnp.where(seat == s, summed / size, means)
        mean_ref[m : m + 1, :] = means
        mine = pltpu.roll(logprob, count - spot, 1)
        token_ref[m : m + 1, :] = mine[:, :toks]


def body(
    hidden_in, layer_gain, router, w_gate, w_up, w_down, final_gain, head, routing, targets, seq_ids
):
    batches, toks, width = hidden_in.shape
    experts = router.shape[2]
    tops = routing.shape[3]
    sections = lax.axis_size("section")
    members = lax.axis_size("expert")
    splits = members // experts // PAIR
    groups = members // PAIR
    cap = min(toks, 9 * toks * tops // (8 * experts))
    dims = (batches, toks, width, experts, splits, tops, cap)
    same_core = [[g * PAIR + c for g in range(groups)] for c in range(PAIR)]
    same_core_all = [
        [s * members + g * PAIR + c for s in range(sections) for g in range(groups)]
        for c in range(PAIR)
    ]
    partner = [(i, i ^ 1) for i in range(members)]
    split = splits * PAIR
    same_place = [[e * split + r for e in range(experts)] for r in range(split)]
    same_place_all = [
        [s * members + e * split + r for s in range(sections) for e in range(experts)]
        for r in range(split)
    ]

    def exchange(rows):
        return lax.all_to_all(
            rows, "expert", split_axis=0, concat_axis=0, axis_index_groups=same_core, tiled=True
        )

    def exchange_all(rows, over):
        return lax.all_to_all(
            rows,
            ("section", "expert"),
            split_axis=0,
            concat_axis=0,
            axis_index_groups=over,
            tiled=True,
        )

    def dispatch_first(rows):
        return lax.all_to_all(
            rows, "expert", split_axis=0, concat_axis=0, axis_index_groups=same_place, tiled=True
        )

    def to_split(rows, shift):
        pairs = []
        for i in range(members):
            place = i // PAIR % splits
            pairs.append((i, i + ((place + shift) % splits - place) * PAIR))
        return lax.ppermute(rows, "expert", pairs)

    def swap_core(rows):
        return lax.ppermute(rows, "expert", partner)

    def by_section(array, shift, across):
        return lax.ppermute(
            array,
            "section",
            [(s, s - s % across + (s + shift) % across) for s in range(sections)],
        )

    early = head.shape[0] * 5 // 8 // 16 * 16
    table_rows = max(-(-(2 + experts) // 8) * 8, toks)
    packed, small, states, early_head = prep(
        dims, table_rows, early, hidden_in, layer_gain, router, routing, final_gain, head
    )
    first_parts = []
    for shift in range(1, batches):
        first_parts.append(by_section(early_head, shift, batches))
    near = dispatch_first(packed)

    shifted = [small]
    for shift in range(1, sections):
        shifted.append(by_section(small, shift, sections))

    inner_size = experts * HALVES * cap
    for tick in range(sections):
        crossing = []
        for shift in range(1, splits):
            crossing.append(to_split(near, shift))
        mixes, gain, *got = ready(
            dims, tick, sections, (w_gate[0], w_up[0], w_down[0]), head, early, states, shifted
        )
        pack = got.pop(0) if tick < sections - 1 else None
        weights = got[:3]
        if tick == 0:
            late_head = got[3]
        mine = [near, *crossing]
        sources = mine + [swap_core(rows) for rows in mine]
        keep, send = expert_rows(dims, tick, sources, weights)
        total = (keep.astype(F32) + swap_core(send).astype(F32)).astype(BF16)
        if sections > batches:
            total = jnp.concatenate([total] * (sections // batches), 0)
        back = exchange_all(total, same_core_all)
        if tick == sections - 1:
            break
        states, packed = advance(dims, tick, back, mixes, states, gain, pack)
        near = exchange_all(packed, same_place_all)
        if sections > batches:
            base = tick + 1 - (tick + 1) % batches
            near = near[base * inner_size : (base + batches) * inner_size]
        if tick == 0:
            near, late_head = lax.optimization_barrier((near, late_head))
            late_parts = []
            for shift in range(1, batches):
                late_parts.append(by_section(late_head, shift, batches))

    (last_rows,) = advance(dims, tick, back, mixes, states, gain, None)
    near = exchange(last_rows)
    far = swap_core(near)
    world = sections * members
    (table,) = call(
        table_kernel,
        [((batches * head.shape[0], width), BF16, True)],
        (head, *first_parts, *late_parts),
        [HBM] + [ANY] * (2 * batches - 2),
        [pltpu.SemaphoreType.DMA((2 * batches - 1,))],
    )
    (stats,) = call(
        lambda *refs: head_kernel(batches, early, *refs),
        [((world, 1, 2 * members * toks), F32)],
        (near, far, targets, table),
        [VMEM] * 4,
        flops=4 * head.size * members * toks,
    )
    stats = lax.all_to_all(stats, ("section", "expert"), split_axis=0, concat_axis=0, tiled=True)
    return call(
        lambda *refs: final_kernel(batches, toks, *refs),
        [((batches, toks), F32), ((batches, SEQS), F32)],
        (stats, seq_ids),
        [VMEM] * 2,
    )


def solution(mesh):
    return jax.shard_map(
        body,
        mesh=mesh,
        in_specs=(
            P(None, "expert", None),
            P("section", None),
            P("section", None, None),
            P("section", None, "expert"),
            P("section", None, "expert"),
            P("section", "expert", None),
            P(),
            P(("section", "expert"), None),
            P("section", None, "expert", None),
            P(),
            P(),
        ),
        out_specs=(P(None, "expert"), P()),
        check_vma=False,
    )
```

```python
import jax
import jax.numpy as jnp
from jax import lax
from jax.experimental import pallas as pl
from jax.experimental.pallas import tpu as pltpu
from jax.sharding import PartitionSpec as P


SEQS = 4
PAIR = 2
HALVES = 2
LANES = 128
MIB = 1024 * 1024
VMEM = pl.BlockSpec(memory_space=pltpu.VMEM)
HBM = pl.BlockSpec(memory_space=pltpu.HBM)
ANY = pl.BlockSpec(memory_space=pl.ANY)
F32 = jnp.float32
BF16 = jnp.bfloat16


def call(kernel, outs, ins, specs, scratch=(), flops=1, vmem=32, moved=None):
    if moved is None:
        moved = sum(a.size * a.dtype.itemsize for a in ins)
    ins = [
        pltpu.with_memory_space_constraint(a, pltpu.HBM) if spec is HBM else a
        for a, spec in zip(ins, specs)
    ]
    return pl.pallas_call(
        kernel,
        out_shape=tuple(
            pltpu.VMEM(*out[:2]) if out[2:] else jax.ShapeDtypeStruct(*out) for out in outs
        ),
        in_specs=specs,
        out_specs=tuple(VMEM for _ in outs),
        scratch_shapes=scratch,
        compiler_params=pltpu.CompilerParams(vmem_limit_bytes=vmem * MIB),
        cost_estimate=pl.CostEstimate(flops=flops, bytes_accessed=moved, transcendentals=0),
    )(*ins)


def iota(shape, dim):
    return lax.broadcasted_iota(jnp.int32, shape, dim)


def dot(a, b, contract=(1, 0)):
    dims = (((contract[0],), (contract[1],)), ((), ()))
    return lax.dot_general(a, b, dims, preferred_element_type=F32)


def places_of(routes, cap):
    toks = routes[0].shape[0]
    lane = iota((toks, LANES), 1)
    named = jnp.zeros((toks, LANES), F32)
    for route in routes:
        named = named + (lane == route).astype(F32)
    earlier = (iota((toks, toks), 1) < iota((toks, toks), 0)).astype(BF16)
    ahead = dot(earlier, named.astype(BF16))
    places = []
    for k, route in enumerate(routes):
        slot = jnp.sum(jnp.where(lane == route, ahead, 0.0), 1, keepdims=True).astype(jnp.int32)
        for other in routes[:k]:
            slot = slot + (other == route).astype(jnp.int32)
        places.append(route * cap + slot)
    return places


def columns(table, start, batches, tops, batch):
    out = []
    for k in range(tops):
        if isinstance(batch, int):
            col = start + batch * tops + k
            out.append(table[:, col : col + 1].astype(jnp.int32))
            continue
        taken = table[:, start + k : start + k + 1]
        for m in range(1, batches):
            col = start + m * tops + k
            taken = jnp.where(batch == m, table[:, col : col + 1], taken)
        out.append(taken.astype(jnp.int32))
    return out


def prep_kernel(dims, *refs):
    sources, head_hbm, refs = refs[:5], refs[5], refs[6:]
    packed_ref, small_ref, states_ref, early_ref = refs[:4]
    held, sems = refs[4:9], refs[9]
    hidden_ref, gain_ref, router_ref, route_ref, final_ref = held
    copies = [pltpu.make_async_copy(*pair, sems.at[i]) for i, pair in enumerate(zip(sources, held))]
    copy = pltpu.make_async_copy(head_hbm.at[pl.ds(0, early_ref.shape[0])], early_ref, sems.at[5])
    for each in copies + [copy]:
        each.start()
    for each in copies:
        each.wait()
    batches, toks, width, experts, _, tops, cap = dims
    wide = width // HALVES
    batch = lax.axis_index("section") % batches
    count = packed_ref.shape[0]
    lane = iota((toks, count), 1)
    lane_place = lane // (batches * cap) * cap + lane % cap
    lane_batch = lane // cap % batches
    picks, normed = [], []
    own = hidden_ref[0]
    eye = (iota((toks, toks), 0) == iota((toks, toks), 1)).astype(F32)
    table = jnp.concatenate(
        [dot(eye, route_ref[m].astype(F32), (1, 1)) for m in range(batches)]
        + [jnp.zeros((toks, LANES - batches * tops), F32)],
        1,
    )
    for m in range(batches):
        hidden = hidden_ref[m]
        values = hidden.astype(F32)
        factor = lax.rsqrt(jnp.mean(values * values, -1, keepdims=True) + 1e-06)
        normed.append((values * factor * gain_ref[...]).astype(BF16))
        hit = jnp.zeros((toks, count), F32)
        for place in places_of(columns(table, 0, batches, tops, m), cap):
            hit = hit + ((lane_place == place) & (lane_batch == m)).astype(F32)
        picks.append(hit.astype(BF16))
        if m:
            own = jnp.where(batch == m, hidden, own)
    packed = dot(jnp.concatenate(picks, 0), jnp.concatenate(normed, 0), (0, 0))
    packed_ref[...] = packed.astype(BF16)
    small_ref[...] = jnp.zeros_like(small_ref)
    small_ref[0:1, 0:width] = gain_ref[...]
    small_ref[1 : 1 + experts, 0:width] = router_ref[...].astype(F32)
    small_ref[1 + experts : 2 + experts, 0:width] = final_ref[...][None, :]
    small_ref[0:toks, width:] = table
    for half in range(HALVES):
        states_ref[half * toks : (half + 1) * toks, :] = own[:, half * wide : (half + 1) * wide]
    copy.wait()


def prep(dims, table_rows, early, hidden_in, layer_gain, router, routing, final_gain, head):
    batches, toks, width, experts, _, _, cap = dims
    arrays = (
        hidden_in,
        layer_gain,
        router[0].T,
        routing[0].transpose(0, 2, 1),
        final_gain,
    )
    return call(
        lambda *refs: prep_kernel(dims, *refs),
        [
            ((experts * batches * cap, width), BF16),
            ((table_rows, width + LANES), F32),
            ((HALVES * toks, width // HALVES), BF16),
            ((early, width), BF16),
        ],
        (*arrays, head),
        [HBM] * 6,
        [pltpu.VMEM(a.shape, a.dtype) for a in arrays] + [pltpu.SemaphoreType.DMA((6,))],
    )


def plan(dims, layer, states, shifted, sections):
    batches, toks, width, experts, splits, tops, cap = dims
    wide = width // HALVES
    section = lax.axis_index("section")
    table = pick_layer(shifted, section, layer, sections)
    routes = columns(table[:toks, width:], 0, batches, tops, section % batches)
    places = places_of(routes, cap)
    values = [states[h * toks : (h + 1) * toks].astype(F32) for h in range(HALVES)]
    square = sum(jnp.sum(v * v, -1, keepdims=True) for v in values)
    factor = lax.rsqrt(square / width + 1e-06)
    logits = 0.0
    for half in range(HALVES):
        cols = slice(half * wide, (half + 1) * wide)
        normed = (values[half] * factor * table[0:1, cols]).astype(BF16)
        logits = logits + dot(normed, table[:, cols].astype(BF16), (1, 1))
    lane = iota(logits.shape, 1)
    scores = [
        jax.nn.sigmoid(jnp.sum(jnp.where(lane == route + 1, logits, 0.0), 1, keepdims=True))
        for route in routes
    ]
    whole = sum(scores)
    count = experts * splits * HALVES * cap
    row = iota((toks, count), 1)
    row_place = row // (splits * HALVES * cap) * cap + row % cap
    row_half = row // cap % HALVES
    mix = jnp.zeros((toks, count), F32)
    for score, place in zip(scores, places):
        mix = mix + jnp.where(row_place == place, 2.5 * (score / whole), 0.0)
    return [jnp.where(row_half == half, mix, 0.0) for half in range(HALVES)]


def pick_layer(shifted, section, layer, sections):
    shift = (section - layer + sections) % sections
    table = shifted[0]
    for k in range(1, sections):
        table = jnp.where(shift == k, shifted[k], table)
    return table


def next_pack(dims, layer, shifted, sections, pack_ref, gain_ref):
    batches, toks, width, experts, _, tops, cap = dims
    wide = width // HALVES
    section = lax.axis_index("section")
    table = pick_layer(shifted, section, layer, sections)
    routes = columns(table[:toks, width:], 0, batches, tops, section % batches)
    count = pack_ref.shape[1]
    row = iota((toks, count), 1)
    row_place = row // (HALVES * cap) % experts * cap + row % cap
    row_half = row // cap % HALVES
    hit = jnp.zeros((toks, count), F32)
    for place in places_of(routes, cap):
        hit = hit + (row_place == place).astype(F32)
    for half in range(HALVES):
        flags = jnp.where(row_half == half, hit, 0.0)
        pack_ref[half * toks : (half + 1) * toks, :] = flags.astype(BF16)
        gain_ref[half : half + 1, :] = table[0:1, half * wide : (half + 1) * wide]


def ready_kernel(dims, layer, sections, *refs):
    _, toks, width, experts, _, _, _ = dims
    last = layer == sections - 1
    wide = width // HALVES
    weights, head_hbm, states_ref = refs[:3], refs[3], refs[4]
    shifted_refs, refs = refs[5 : 5 + sections], refs[5 + sections :]
    mix_ref, gain_ref, refs = refs[0], refs[1], refs[2:]
    if not last:
        pack_ref, refs = refs[0], refs[1:]
    held, sems = refs[:3], refs[-1]
    copies = [pltpu.make_async_copy(*pair, sems.at[i]) for i, pair in enumerate(zip(weights, held))]
    if layer == 0:
        late = refs[3].shape[0]
        rest = pl.ds(head_hbm.shape[0] - late, late)
        copies.append(pltpu.make_async_copy(head_hbm.at[rest], refs[3], sems.at[len(weights)]))
    for copy in copies:
        copy.start()

    shifted = [ref[...] for ref in shifted_refs]
    for half, mix in enumerate(plan(dims, layer, states_ref[...], shifted, sections)):
        high = mix.astype(BF16)
        mix_ref[half * toks : (half + 1) * toks, :] = high
        low = (mix - high.astype(F32)).astype(BF16)
        mix_ref[(HALVES + half) * toks : (HALVES + half + 1) * toks, :] = low
    if last:
        for half in range(HALVES):
            cols = slice(half * wide, (half + 1) * wide)
            gain_ref[half : half + 1, :] = shifted[0][1 + experts : 2 + experts, cols]
    else:
        next_pack(dims, layer + 1, shifted, sections, pack_ref, gain_ref)

    for copy in copies:
        copy.wait()


def ready(dims, layer, sections, weights, head, early, states, shifted):
    _, toks, width, experts, splits, _, cap = dims
    back = experts * splits * HALVES * cap
    outs = [((2 * HALVES * toks, back), BF16), ((HALVES, width // HALVES), F32)]
    if layer < sections - 1:
        outs.append(((HALVES * toks, sections * experts * HALVES * cap), BF16))
    outs += [(weight.shape, BF16, True) for weight in weights]
    if layer == 0:
        outs.append(((head.shape[0] - early, width), BF16))
    return call(
        lambda *refs: ready_kernel(dims, layer, sections, *refs),
        outs,
        (*weights, head, states, *shifted),
        [HBM] * 4 + [VMEM] * (1 + sections),
        [pltpu.SemaphoreType.DMA((4,))],
    )


def expert_kernel(dims, split, *refs):
    batches, _, _, experts, splits, _, cap = dims
    sources, refs = refs[: PAIR * splits], refs[PAIR * splits :]
    gate_ref, up_ref, down_ref, keep_ref, send_ref = refs
    count, wide = keep_ref.shape
    rows = count // HALVES
    each = rows // splits
    place = lax.axis_index("expert") // PAIR % splits

    fast = HALVES * cap == 8 and experts % 2 == 0 and (split or batches * cap == 8)
    turn = HALVES * cap // 2

    def low(shape):
        return iota(shape, 1) < turn

    def whole(ref):
        if not split:
            return ref[...]
        if fast:
            blocks = ref[...].astype(F32).reshape(each // 8, 2, 8, wide)
            first, second = blocks[:, 0], blocks[:, 1]
            low_half = low(first.shape)
            left = jnp.where(low_half, first, pltpu.roll(second, turn, 1))
            right = jnp.where(low_half, pltpu.roll(first, turn, 1), second)
            parts = [left.reshape(each, wide).astype(BF16), right.reshape(each, wide).astype(BF16)]
            return jnp.concatenate(parts, 1)
        shape = (each, HALVES * each)
        row, col = iota(shape, 0), iota(shape, 1)
        parts = []
        for half in range(HALVES):
            pick = row // cap * (HALVES * cap) + half * cap + row % cap == col
            parts.append(dot(pick.astype(BF16), ref[...]).astype(BF16))
        return jnp.concatenate(parts, 1)

    row, col = iota((count, rows), 0), iota((count, rows), 1)
    slot, side = row % cap, row // cap % HALVES
    shift = (place - row // (HALVES * cap) % splits + splits) % splits
    block = row // (HALVES * cap * splits)
    if not split:
        block = block % experts * batches + block // experts
    source = shift * each + block * cap + slot
    data = jnp.concatenate([whole(ref) for ref in sources], 0)
    gate_val, up_val = dot(data, gate_ref[...]), dot(data, up_ref[...])
    inner = (gate_val / (1.0 + jnp.exp(-gate_val)) * up_val).astype(BF16)
    if fast:
        left, right = (dot(inner, down_ref[:, h * wide : (h + 1) * wide]) for h in range(HALVES))
        for core, ref in ((1, send_ref), (0, keep_ref)):
            moved = []
            for k in range(splits):
                part = slice(core * rows + k * each, core * rows + (k + 1) * each)
                a = left[part].reshape(each // 8, 8, wide)
                b = right[part].reshape(each // 8, 8, wide)
                low_half = low(a.shape)
                first = jnp.where(low_half, a, pltpu.roll(b, turn, 1))
                moved.append((first, jnp.where(low_half, pltpu.roll(a, turn, 1), b)))
            for index in range(batches * experts):
                if split:
                    which, at = index % 2, index // 2
                else:
                    which, at = index // experts, index % experts
                for h in range(splits):
                    taken = moved[0][which][at]
                    for k in range(1, splits):
                        taken = jnp.where((place - h + splits) % splits == k, moved[k][which][at], taken)
                    ref[(index * splits + h) * 8 : (index * splits + h + 1) * 8, :] = taken.astype(BF16)
        return
    keep = send = 0.0
    for half in range(HALVES):
        part = dot(inner, down_ref[:, half * wide : (half + 1) * wide]).astype(BF16)
        pick = ((source == col) & (side == half)).astype(BF16)
        send = send + dot(pick, part[rows:])
        keep = keep + dot(pick, part[:rows])
    send_ref[...] = send.astype(BF16)
    keep_ref[...] = keep.astype(BF16)


def expert_rows(dims, layer, sources, weights):
    batches, _, width, experts, splits, _, cap = dims
    count = batches * experts * splits * HALVES * cap
    return call(
        lambda *refs: expert_kernel(dims, layer > 0, *refs),
        [((count, width // HALVES), BF16)] * 2,
        (*sources, *weights),
        [VMEM] * (len(sources) + 3),
        flops=6 * count * width * weights[0].shape[1],
    )


def advance_kernel(dims, layer, last, back_ref, mix_ref, states_ref, gain_ref, *refs):
    _, toks, width, _, _, _, _ = dims
    wide = width // HALVES
    size = mix_ref.shape[1]
    mixed = dot(mix_ref[...], back_ref[layer * size : (layer + 1) * size, :])
    states = states_ref[...].astype(F32) + mixed[: HALVES * toks] + mixed[HALVES * toks :]
    states = states.astype(BF16)
    values = states.astype(F32)
    square = jnp.sum(values * values, -1, keepdims=True)
    factor = lax.rsqrt(sum(square[h * toks : (h + 1) * toks] for h in range(HALVES)) / width + 1e-06)
    normed = [
        (values[h * toks : (h + 1) * toks] * factor * gain_ref[h : h + 1, :]).astype(BF16)
        for h in range(HALVES)
    ]
    if last:
        out_ref = refs[0]
        for h in range(HALVES):
            for copy in range(out_ref.shape[0] // toks):
                out_ref[copy * toks : (copy + 1) * toks, h * wide : (h + 1) * wide] = normed[h]
        return
    pack_ref, out_ref, packed_ref = refs
    out_ref[...] = states
    packed_ref[...] = dot(pack_ref[...], jnp.concatenate(normed, 0), (0, 0)).astype(BF16)


def advance(dims, layer, back, mixes, states, gain, pack):
    _, toks, width, experts, splits, _, _ = dims
    last = pack is None
    if last:
        outs = [((experts * splits * toks, width), BF16)]
    else:
        outs = [(states.shape, BF16), ((pack.shape[1], width // HALVES), BF16)]
    ins = (back, mixes, states, gain) + (() if last else (pack,))
    return call(
        lambda *refs: advance_kernel(dims, layer, last, *refs), outs, ins, [VMEM] * len(ins)
    )


def table_kernel(*refs):
    sources, table_ref, sems = refs[:-2], refs[-2], refs[-1]
    copies, spot = [], 0
    for i, source in enumerate(sources):
        size = source.shape[0]
        copies.append(pltpu.make_async_copy(source, table_ref.at[pl.ds(spot, size)], sems.at[i]))
        spot += size
    for copy in copies:
        copy.start()
    for copy in copies:
        copy.wait()


def head_kernel(batches, early, near_ref, far_ref, target_ref, table_ref, out_ref):
    others = batches - 1
    vocab = table_ref.shape[0] // batches
    section, member = lax.axis_index("section"), lax.axis_index("expert")
    members = lax.axis_size("expert")
    batch = section % batches
    toks = near_ref.shape[0] + far_ref.shape[0]
    each = toks // members
    col = iota((toks, toks), 1)
    core = (col // (toks // PAIR) + member) % PAIR
    moved = iota((toks, toks), 0) == (col // each % (members // PAIR) * PAIR + core) * each + col % each
    moved = moved.astype(F32)
    ids = target_ref[...].astype(F32)
    target = ids[0:1]
    for m in range(1, batches):
        target = jnp.where(batch == m, ids[m : m + 1], target)
    exact = lax.Precision.HIGHEST
    target = jnp.broadcast_to(target, (8, toks))
    target = jnp.dot(target, moved, precision=exact, preferred_element_type=F32)[0:1].astype(jnp.int32)

    rows = jnp.concatenate([near_ref[...], far_ref[...]], 0)
    logits = dot(table_ref[...], rows, (1, 1))
    blocks, spot = [(logits[:vocab], (section * members + member) * vocab)], vocab
    for i in range(2 * others):
        size = early if i < others else vocab - early
        owner = section - batch + (batch - i % others - 1 + batches) % batches
        start = (owner * members + member) * vocab + (early if i >= others else 0)
        blocks.append((logits[spot : spot + size], start))
        spot += size
    peak = blocks[0][0].max(0, keepdims=True)
    for block, _ in blocks[1:]:
        peak = jnp.maximum(peak, block.max(0, keepdims=True))
    total = hit = 0.0
    for block, start in blocks:
        total = total + jnp.sum(jnp.exp(block - peak), 0, keepdims=True)
        hit = hit + jnp.sum(jnp.where(iota(block.shape, 0) + start == target, block, 0.0), 0, keepdims=True)
    both = jnp.concatenate([peak + jnp.log(total), hit, jnp.zeros((6, toks), F32)], 0)
    both = lax.dot_general(
        both, moved, (((1,), (1,)), ((), ())), precision=exact, preferred_element_type=F32
    )
    out = jnp.concatenate([both[0:1], both[1:2]], 1)
    out_ref[...] = jnp.broadcast_to(out[None], out_ref.shape)


def final_kernel(batches, toks, stats_ref, seq_ref, token_ref, mean_ref):
    member = lax.axis_index("expert")
    members = lax.axis_size("expert")
    sections = lax.axis_size("section")
    count = members * toks
    stats = stats_ref[:, 0, :]
    spot = member * toks
    lane = iota((1, count), 1)
    seat = iota((1, SEQS), 1)
    for m in range(batches):
        rows = [stats[s * members : (s + 1) * members] for s in range(m, sections, batches)]
        rows = rows[0] if len(rows) == 1 else jnp.concatenate(rows, 0)
        local, hits = rows[:, :count], rows[:, count:]
        peak = jnp.max(local, 0, keepdims=True)
        lse = peak + jnp.log(jnp.sum(jnp.exp(local - peak), 0, keepdims=True))
        logprob = jnp.sum(hits, 0, keepdims=True) - lse
        ids = seq_ref[m : m + 1, :]
        means = jnp.zeros((1, SEQS), F32)
        for s in range(SEQS):
            inside = ids == s
            summed = jnp.sum(jnp.where(inside, logprob, 0.0), 1, keepdims=True)
            size = jnp.sum(jnp.where(inside, 1.0, 0.0), 1, keepdims=True)
            means = jnp.where(seat == s, summed / size, means)
        mean_ref[m : m + 1, :] = means
        mine = pltpu.roll(logprob, count - spot, 1)
        token_ref[m : m + 1, :] = mine[:, :toks]


def body(
    hidden_in, layer_gain, router, w_gate, w_up, w_down, final_gain, head, routing, targets, seq_ids
):
    batches, toks, width = hidden_in.shape
    experts = router.shape[2]
    tops = routing.shape[3]
    sections = lax.axis_size("section")
    members = lax.axis_size("expert")
    splits = members // experts // PAIR
    groups = members // PAIR
    cap = min(toks, 9 * toks * tops // (8 * experts))
    dims = (batches, toks, width, experts, splits, tops, cap)
    same_core = [[g * PAIR + c for g in range(groups)] for c in range(PAIR)]
    same_core_all = [
        [s * members + g * PAIR + c for s in range(sections) for g in range(groups)]
        for c in range(PAIR)
    ]
    partner = [(i, i ^ 1) for i in range(members)]
    split = splits * PAIR
    same_place = [[e * split + r for e in range(experts)] for r in range(split)]
    same_place_all = [
        [s * members + e * split + r for s in range(sections) for e in range(experts)]
        for r in range(split)
    ]

    def exchange(rows):
        return lax.all_to_all(
            rows, "expert", split_axis=0, concat_axis=0, axis_index_groups=same_core, tiled=True
        )

    def exchange_all(rows, over):
        return lax.all_to_all(
            rows,
            ("section", "expert"),
            split_axis=0,
            concat_axis=0,
            axis_index_groups=over,
            tiled=True,
        )

    def dispatch_first(rows):
        return lax.all_to_all(
            rows, "expert", split_axis=0, concat_axis=0, axis_index_groups=same_place, tiled=True
        )

    def to_split(rows, shift):
        pairs = []
        for i in range(members):
            place = i // PAIR % splits
            pairs.append((i, i + ((place + shift) % splits - place) * PAIR))
        return lax.ppermute(rows, "expert", pairs)

    def swap_core(rows):
        return lax.ppermute(rows, "expert", partner)

    def by_section(array, shift, across):
        return lax.ppermute(
            array,
            "section",
            [(s, s - s % across + (s + shift) % across) for s in range(sections)],
        )

    early = head.shape[0] * 5 // 8 // 16 * 16
    table_rows = max(-(-(2 + experts) // 8) * 8, toks)
    packed, small, states, early_head = prep(
        dims, table_rows, early, hidden_in, layer_gain, router, routing, final_gain, head
    )
    first_parts = []
    for shift in range(1, batches):
        first_parts.append(by_section(early_head, shift, batches))
    near = dispatch_first(packed)

    shifted = [small]
    for shift in range(1, sections):
        shifted.append(by_section(small, shift, sections))

    inner_size = experts * HALVES * cap
    for tick in range(sections):
        crossing = []
        for shift in range(1, splits):
            crossing.append(to_split(near, shift))
        mixes, gain, *got = ready(
            dims, tick, sections, (w_gate[0], w_up[0], w_down[0]), head, early, states, shifted
        )
        pack = got.pop(0) if tick < sections - 1 else None
        weights = got[:3]
        if tick == 0:
            late_head = got[3]
        mine = [near, *crossing]
        sources = mine + [swap_core(rows) for rows in mine]
        keep, send = expert_rows(dims, tick, sources, weights)
        total = (keep.astype(F32) + swap_core(send).astype(F32)).astype(BF16)
        if sections > batches:
            total = jnp.concatenate([total] * (sections // batches), 0)
        back = exchange_all(total, same_core_all)
        if tick == sections - 1:
            break
        states, packed = advance(dims, tick, back, mixes, states, gain, pack)
        near = exchange_all(packed, same_place_all)
        if sections > batches:
            base = tick + 1 - (tick + 1) % batches
            near = near[base * inner_size : (base + batches) * inner_size]
        if tick == 0:
            near, late_head = lax.optimization_barrier((near, late_head))
            late_parts = []
            for shift in range(1, batches):
                late_parts.append(by_section(late_head, shift, batches))

    (last_rows,) = advance(dims, tick, back, mixes, states, gain, None)
    near = exchange(last_rows)
    far = swap_core(near)
    world = sections * members
    (table,) = call(
        table_kernel,
        [((batches * head.shape[0], width), BF16, True)],
        (head, *first_parts, *late_parts),
        [HBM] + [ANY] * (2 * batches - 2),
        [pltpu.SemaphoreType.DMA((2 * batches - 1,))],
    )
    (stats,) = call(
        lambda *refs: head_kernel(batches, early, *refs),
        [((world, 1, 2 * members * toks), F32)],
        (near, far, targets, table),
        [VMEM] * 4,
        flops=4 * head.size * members * toks,
    )
    stats = lax.all_to_all(stats, ("section", "expert"), split_axis=0, concat_axis=0, tiled=True)
    return call(
        lambda *refs: final_kernel(batches, toks, *refs),
        [((batches, toks), F32), ((batches, SEQS), F32)],
        (stats, seq_ids),
        [VMEM] * 2,
    )


def solution(mesh):
    return jax.shard_map(
        body,
        mesh=mesh,
        in_specs=(
            P(None, "expert", None),
            P("section", None),
            P("section", None, None),
            P("section", None, "expert"),
            P("section", None, "expert"),
            P("section", "expert", None),
            P(),
            P(("section", "expert"), None),
            P("section", None, "expert", None),
            P(),
            P(),
        ),
        out_specs=(P(None, "expert"), P()),
        check_vma=False,
    )
```

```python
import jax
import jax.numpy as jnp
from jax import lax
from jax.experimental import pallas as pl
from jax.experimental.pallas import tpu as pltpu
from jax.sharding import PartitionSpec as P


SEQS = 4
PAIR = 2
HALVES = 2
LANES = 128
MIB = 1024 * 1024
VMEM = pl.BlockSpec(memory_space=pltpu.VMEM)
HBM = pl.BlockSpec(memory_space=pltpu.HBM)
ANY = pl.BlockSpec(memory_space=pl.ANY)
F32 = jnp.float32
BF16 = jnp.bfloat16


def call(kernel, outs, ins, specs, scratch=(), flops=1, vmem=32, moved=None):
    if moved is None:
        moved = sum(a.size * a.dtype.itemsize for a in ins)
    ins = [
        pltpu.with_memory_space_constraint(a, pltpu.HBM) if spec is HBM else a
        for a, spec in zip(ins, specs)
    ]
    return pl.pallas_call(
        kernel,
        out_shape=tuple(
            pltpu.VMEM(*out[:2]) if out[2:] else jax.ShapeDtypeStruct(*out) for out in outs
        ),
        in_specs=specs,
        out_specs=tuple(VMEM for _ in outs),
        scratch_shapes=scratch,
        compiler_params=pltpu.CompilerParams(vmem_limit_bytes=vmem * MIB),
        cost_estimate=pl.CostEstimate(flops=flops, bytes_accessed=moved, transcendentals=0),
    )(*ins)


def iota(shape, dim):
    return lax.broadcasted_iota(jnp.int32, shape, dim)


def dot(a, b, contract=(1, 0)):
    dims = (((contract[0],), (contract[1],)), ((), ()))
    return lax.dot_general(a, b, dims, preferred_element_type=F32)


def places_of(routes, cap):
    toks = routes[0].shape[0]
    lane = iota((toks, LANES), 1)
    named = jnp.zeros((toks, LANES), F32)
    for route in routes:
        named = named + (lane == route).astype(F32)
    earlier = (iota((toks, toks), 1) < iota((toks, toks), 0)).astype(BF16)
    ahead = dot(earlier, named.astype(BF16))
    places = []
    for k, route in enumerate(routes):
        slot = jnp.sum(jnp.where(lane == route, ahead, 0.0), 1, keepdims=True).astype(jnp.int32)
        for other in routes[:k]:
            slot = slot + (other == route).astype(jnp.int32)
        places.append(route * cap + slot)
    return places


def columns(table, start, batches, tops, batch):
    out = []
    for k in range(tops):
        if isinstance(batch, int):
            col = start + batch * tops + k
            out.append(table[:, col : col + 1].astype(jnp.int32))
            continue
        taken = table[:, start + k : start + k + 1]
        for m in range(1, batches):
            col = start + m * tops + k
            taken = jnp.where(batch == m, table[:, col : col + 1], taken)
        out.append(taken.astype(jnp.int32))
    return out


def prep_kernel(dims, *refs):
    sources, head_hbm, refs = refs[:5], refs[5], refs[6:]
    packed_ref, small_ref, states_ref, early_ref = refs[:4]
    held, sems = refs[4:9], refs[9]
    hidden_ref, gain_ref, router_ref, route_ref, final_ref = held
    copies = [pltpu.make_async_copy(*pair, sems.at[i]) for i, pair in enumerate(zip(sources, held))]
    copy = pltpu.make_async_copy(head_hbm.at[pl.ds(0, early_ref.shape[0])], early_ref, sems.at[5])
    for each in copies + [copy]:
        each.start()
    for each in copies:
        each.wait()
    batches, toks, width, experts, _, tops, cap = dims
    wide = width // HALVES
    batch = lax.axis_index("section") % batches
    count = packed_ref.shape[0]
    lane = iota((toks, count), 1)
    lane_place = lane // (batches * cap) * cap + lane % cap
    lane_batch = lane // cap % batches
    picks, normed = [], []
    own = hidden_ref[0]
    eye = (iota((toks, toks), 0) == iota((toks, toks), 1)).astype(F32)
    table = jnp.concatenate(
        [dot(eye, route_ref[m].astype(F32), (1, 1)) for m in range(batches)]
        + [jnp.zeros((toks, LANES - batches * tops), F32)],
        1,
    )
    for m in range(batches):
        hidden = hidden_ref[m]
        values = hidden.astype(F32)
        factor = lax.rsqrt(jnp.mean(values * values, -1, keepdims=True) + 1e-06)
        normed.append((values * factor * gain_ref[...]).astype(BF16))
        hit = jnp.zeros((toks, count), F32)
        for place in places_of(columns(table, 0, batches, tops, m), cap):
            hit = hit + ((lane_place == place) & (lane_batch == m)).astype(F32)
        picks.append(hit.astype(BF16))
        if m:
            own = jnp.where(batch == m, hidden, own)
    packed = dot(jnp.concatenate(picks, 0), jnp.concatenate(normed, 0), (0, 0))
    packed_ref[...] = packed.astype(BF16)
    small_ref[...] = jnp.zeros_like(small_ref)
    small_ref[0:1, 0:width] = gain_ref[...]
    small_ref[1 : 1 + experts, 0:width] = router_ref[...].astype(F32)
    small_ref[1 + experts : 2 + experts, 0:width] = final_ref[...][None, :]
    small_ref[0:toks, width:] = table
    for half in range(HALVES):
        states_ref[half * toks : (half + 1) * toks, :] = own[:, half * wide : (half + 1) * wide]
    copy.wait()


def prep(dims, table_rows, early, hidden_in, layer_gain, router, routing, final_gain, head):
    batches, toks, width, experts, _, _, cap = dims
    arrays = (
        hidden_in,
        layer_gain,
        router[0].T,
        routing[0].transpose(0, 2, 1),
        final_gain,
    )
    return call(
        lambda *refs: prep_kernel(dims, *refs),
        [
            ((experts * batches * cap, width), BF16),
            ((table_rows, width + LANES), F32),
            ((HALVES * toks, width // HALVES), BF16),
            ((early, width), BF16),
        ],
        (*arrays, head),
        [HBM] * 6,
        [pltpu.VMEM(a.shape, a.dtype) for a in arrays] + [pltpu.SemaphoreType.DMA((6,))],
    )


def plan(dims, layer, states, shifted, sections):
    batches, toks, width, experts, splits, tops, cap = dims
    wide = width // HALVES
    section = lax.axis_index("section")
    table = pick_layer(shifted, section, layer, sections)
    routes = columns(table[:toks, width:], 0, batches, tops, section % batches)
    places = places_of(routes, cap)
    values = [states[h * toks : (h + 1) * toks].astype(F32) for h in range(HALVES)]
    square = sum(jnp.sum(v * v, -1, keepdims=True) for v in values)
    factor = lax.rsqrt(square / width + 1e-06)
    logits = 0.0
    for half in range(HALVES):
        cols = slice(half * wide, (half + 1) * wide)
        normed = (values[half] * factor * table[0:1, cols]).astype(BF16)
        logits = logits + dot(normed, table[:, cols].astype(BF16), (1, 1))
    lane = iota(logits.shape, 1)
    scores = [
        jax.nn.sigmoid(jnp.sum(jnp.where(lane == route + 1, logits, 0.0), 1, keepdims=True))
        for route in routes
    ]
    whole = sum(scores)
    count = experts * splits * HALVES * cap
    row = iota((toks, count), 1)
    row_place = row // (splits * HALVES * cap) * cap + row % cap
    row_half = row // cap % HALVES
    mix = jnp.zeros((toks, count), F32)
    for score, place in zip(scores, places):
        mix = mix + jnp.where(row_place == place, 2.5 * (score / whole), 0.0)
    return [jnp.where(row_half == half, mix, 0.0) for half in range(HALVES)]


def pick_layer(shifted, section, layer, sections):
    shift = (section - layer + sections) % sections
    table = shifted[0]
    for k in range(1, sections):
        table = jnp.where(shift == k, shifted[k], table)
    return table


def next_pack(dims, layer, shifted, sections, pack_ref, gain_ref):
    batches, toks, width, experts, _, tops, cap = dims
    wide = width // HALVES
    section = lax.axis_index("section")
    table = pick_layer(shifted, section, layer, sections)
    routes = columns(table[:toks, width:], 0, batches, tops, section % batches)
    count = pack_ref.shape[1]
    row = iota((toks, count), 1)
    row_place = row // (HALVES * cap) % experts * cap + row % cap
    row_half = row // cap % HALVES
    hit = jnp.zeros((toks, count), F32)
    for place in places_of(routes, cap):
        hit = hit + (row_place == place).astype(F32)
    for half in range(HALVES):
        flags = jnp.where(row_half == half, hit, 0.0)
        pack_ref[half * toks : (half + 1) * toks, :] = flags.astype(BF16)
        gain_ref[half : half + 1, :] = table[0:1, half * wide : (half + 1) * wide]


def ready_kernel(dims, layer, sections, *refs):
    _, toks, width, experts, _, _, _ = dims
    last = layer == sections - 1
    wide = width // HALVES
    weights, head_hbm, states_ref = refs[:3], refs[3], refs[4]
    shifted_refs, refs = refs[5 : 5 + sections], refs[5 + sections :]
    mix_ref, gain_ref, refs = refs[0], refs[1], refs[2:]
    if not last:
        pack_ref, refs = refs[0], refs[1:]
    held, sems = refs[:3], refs[-1]
    copies = [pltpu.make_async_copy(*pair, sems.at[i]) for i, pair in enumerate(zip(weights, held))]
    if layer == 0:
        late = refs[3].shape[0]
        rest = pl.ds(head_hbm.shape[0] - late, late)
        copies.append(pltpu.make_async_copy(head_hbm.at[rest], refs[3], sems.at[len(weights)]))
    for copy in copies:
        copy.start()

    shifted = [ref[...] for ref in shifted_refs]
    for half, mix in enumerate(plan(dims, layer, states_ref[...], shifted, sections)):
        high = mix.astype(BF16)
        mix_ref[half * toks : (half + 1) * toks, :] = high
        low = (mix - high.astype(F32)).astype(BF16)
        mix_ref[(HALVES + half) * toks : (HALVES + half + 1) * toks, :] = low
    if last:
        for half in range(HALVES):
            cols = slice(half * wide, (half + 1) * wide)
            gain_ref[half : half + 1, :] = shifted[0][1 + experts : 2 + experts, cols]
    else:
        next_pack(dims, layer + 1, shifted, sections, pack_ref, gain_ref)

    for copy in copies:
        copy.wait()


def ready(dims, layer, sections, weights, head, early, states, shifted):
    _, toks, width, experts, splits, _, cap = dims
    back = experts * splits * HALVES * cap
    outs = [((2 * HALVES * toks, back), BF16), ((HALVES, width // HALVES), F32)]
    if layer < sections - 1:
        outs.append(((HALVES * toks, sections * experts * HALVES * cap), BF16))
    outs += [(weight.shape, BF16, True) for weight in weights]
    if layer == 0:
        outs.append(((head.shape[0] - early, width), BF16))
    return call(
        lambda *refs: ready_kernel(dims, layer, sections, *refs),
        outs,
        (*weights, head, states, *shifted),
        [HBM] * 4 + [VMEM] * (1 + sections),
        [pltpu.SemaphoreType.DMA((4,))],
    )


def expert_kernel(dims, split, *refs):
    batches, _, _, experts, splits, _, cap = dims
    sources, refs = refs[: PAIR * splits], refs[PAIR * splits :]
    gate_ref, up_ref, down_ref, keep_ref, send_ref = refs
    count, wide = keep_ref.shape
    rows = count // HALVES
    each = rows // splits
    place = lax.axis_index("expert") // PAIR % splits

    fast = HALVES * cap == 8 and experts % 2 == 0 and (split or batches * cap == 8)
    turn = HALVES * cap // 2

    def low(shape):
        return iota(shape, 1) < turn

    def whole(ref):
        if not split:
            return ref[...]
        if fast:
            blocks = ref[...].astype(F32).reshape(each // 8, 2, 8, wide)
            first, second = blocks[:, 0], blocks[:, 1]
            low_half = low(first.shape)
            left = jnp.where(low_half, first, pltpu.roll(second, turn, 1))
            right = jnp.where(low_half, pltpu.roll(first, turn, 1), second)
            parts = [left.reshape(each, wide).astype(BF16), right.reshape(each, wide).astype(BF16)]
            return jnp.concatenate(parts, 1)
        shape = (each, HALVES * each)
        row, col = iota(shape, 0), iota(shape, 1)
        parts = []
        for half in range(HALVES):
            pick = row // cap * (HALVES * cap) + half * cap + row % cap == col
            parts.append(dot(pick.astype(BF16), ref[...]).astype(BF16))
        return jnp.concatenate(parts, 1)

    row, col = iota((count, rows), 0), iota((count, rows), 1)
    slot, side = row % cap, row // cap % HALVES
    shift = (place - row // (HALVES * cap) % splits + splits) % splits
    block = row // (HALVES * cap * splits)
    if not split:
        block = block % experts * batches + block // experts
    source = shift * each + block * cap + slot
    data = jnp.concatenate([whole(ref) for ref in sources], 0)
    gate_val, up_val = dot(data, gate_ref[...]), dot(data, up_ref[...])
    inner = (gate_val / (1.0 + jnp.exp(-gate_val)) * up_val).astype(BF16)
    if fast:
        left, right = (dot(inner, down_ref[:, h * wide : (h + 1) * wide]) for h in range(HALVES))
        for core, ref in ((1, send_ref), (0, keep_ref)):
            moved = []
            for k in range(splits):
                part = slice(core * rows + k * each, core * rows + (k + 1) * each)
                a = left[part].reshape(each // 8, 8, wide)
                b = right[part].reshape(each // 8, 8, wide)
                low_half = low(a.shape)
                first = jnp.where(low_half, a, pltpu.roll(b, turn, 1))
                moved.append((first, jnp.where(low_half, pltpu.roll(a, turn, 1), b)))
            for index in range(batches * experts):
                if split:
                    which, at = index % 2, index // 2
                else:
                    which, at = index // experts, index % experts
                for h in range(splits):
                    taken = moved[0][which][at]
                    for k in range(1, splits):
                        taken = jnp.where((place - h + splits) % splits == k, moved[k][which][at], taken)
                    ref[(index * splits + h) * 8 : (index * splits + h + 1) * 8, :] = taken.astype(BF16)
        return
    keep = send = 0.0
    for half in range(HALVES):
        part = dot(inner, down_ref[:, half * wide : (half + 1) * wide]).astype(BF16)
        pick = ((source == col) & (side == half)).astype(BF16)
        send = send + dot(pick, part[rows:])
        keep = keep + dot(pick, part[:rows])
    send_ref[...] = send.astype(BF16)
    keep_ref[...] = keep.astype(BF16)


def expert_rows(dims, layer, sources, weights):
    batches, _, width, experts, splits, _, cap = dims
    count = batches * experts * splits * HALVES * cap
    return call(
        lambda *refs: expert_kernel(dims, layer > 0, *refs),
        [((count, width // HALVES), BF16)] * 2,
        (*sources, *weights),
        [VMEM] * (len(sources) + 3),
        flops=6 * count * width * weights[0].shape[1],
    )


def advance_kernel(dims, layer, last, back_ref, mix_ref, states_ref, gain_ref, *refs):
    _, toks, width, _, _, _, _ = dims
    wide = width // HALVES
    size = mix_ref.shape[1]
    mixed = dot(mix_ref[...], back_ref[layer * size : (layer + 1) * size, :])
    states = states_ref[...].astype(F32) + mixed[: HALVES * toks] + mixed[HALVES * toks :]
    states = states.astype(BF16)
    values = states.astype(F32)
    square = jnp.sum(values * values, -1, keepdims=True)
    factor = lax.rsqrt(sum(square[h * toks : (h + 1) * toks] for h in range(HALVES)) / width + 1e-06)
    normed = [
        (values[h * toks : (h + 1) * toks] * factor * gain_ref[h : h + 1, :]).astype(BF16)
        for h in range(HALVES)
    ]
    if last:
        out_ref = refs[0]
        for h in range(HALVES):
            for copy in range(out_ref.shape[0] // toks):
                out_ref[copy * toks : (copy + 1) * toks, h * wide : (h + 1) * wide] = normed[h]
        return
    pack_ref, out_ref, packed_ref = refs
    out_ref[...] = states
    packed_ref[...] = dot(pack_ref[...], jnp.concatenate(normed, 0), (0, 0)).astype(BF16)


def advance(dims, layer, back, mixes, states, gain, pack):
    _, toks, width, experts, splits, _, _ = dims
    last = pack is None
    if last:
        outs = [((experts * splits * toks, width), BF16)]
    else:
        outs = [(states.shape, BF16), ((pack.shape[1], width // HALVES), BF16)]
    ins = (back, mixes, states, gain) + (() if last else (pack,))
    return call(lambda *refs: advance_kernel(dims, layer, last, *refs), outs, ins, [VMEM] * len(ins))


def table_kernel(batches, toks, target_ref, *refs):
    sources, table_ref, moved_ref, wanted_ref, sems = refs[:-4], *refs[-4:]
    copies, spot = [], 0
    for i, source in enumerate(sources):
        size = source.shape[0]
        copies.append(pltpu.make_async_copy(source, table_ref.at[pl.ds(spot, size)], sems.at[i]))
        spot += size
    for copy in copies:
        copy.start()

    member = lax.axis_index("expert")
    members = lax.axis_size("expert")
    batch = lax.axis_index("section") % batches
    each = toks // members
    col = iota((toks, toks), 1)
    core = (col // (toks // PAIR) + member) % PAIR
    moved = iota((toks, toks), 0) == (col // each % (members // PAIR) * PAIR + core) * each + col % each
    moved = moved.astype(F32).astype(BF16)
    moved_ref[...] = moved
    ids = target_ref[...]
    target = ids[0:1]
    for m in range(1, batches):
        target = jnp.where(batch == m, ids[m : m + 1], target)
    high, low = target // 256, target % 256
    digits = jnp.concatenate([high, low, jnp.zeros((6, toks), jnp.int32)], 0).astype(F32).astype(BF16)
    placed = dot(digits, moved)
    wanted_ref[...] = (placed[0:1] * 256.0 + placed[1:2]).astype(jnp.int32)
    for copy in copies:
        copy.wait()


def head_kernel(batches, early, near_ref, far_ref, table_ref, moved_ref, wanted_ref, out_ref):
    others = batches - 1
    vocab = table_ref.shape[0] // batches
    section, member = lax.axis_index("section"), lax.axis_index("expert")
    members = lax.axis_size("expert")
    batch = section % batches
    toks = near_ref.shape[0] + far_ref.shape[0]
    moved, target = moved_ref[...], wanted_ref[...]
    rows = jnp.concatenate([near_ref[...], far_ref[...]], 0)
    logits = dot(table_ref[...], rows, (1, 1))
    blocks, spot = [(logits[:vocab], (section * members + member) * vocab)], vocab
    for i in range(2 * others):
        size = early if i < others else vocab - early
        owner = section - batch + (batch - i % others - 1 + batches) % batches
        start = (owner * members + member) * vocab + (early if i >= others else 0)
        blocks.append((logits[spot : spot + size], start))
        spot += size
    peak = blocks[0][0].max(0, keepdims=True)
    for block, _ in blocks[1:]:
        peak = jnp.maximum(peak, block.max(0, keepdims=True))
    total = hit = 0.0
    for block, start in blocks:
        total = total + jnp.sum(jnp.exp(block - peak), 0, keepdims=True)
        hit = hit + jnp.sum(jnp.where(iota(block.shape, 0) + start == target, block, 0.0), 0, keepdims=True)
    rest = jnp.concatenate([peak + jnp.log(total), hit], 0)
    pieces = []
    for _ in range(3):
        pieces.append(rest.astype(BF16))
        rest = rest - pieces[-1].astype(F32)
    whole = dot(jnp.concatenate(pieces + [jnp.zeros((2, toks), BF16)], 0), moved, (1, 1))
    both = whole[0:2] + whole[2:4] + whole[4:6]
    out = jnp.concatenate([both[0:1], both[1:2]], 1)
    out_ref[...] = jnp.broadcast_to(out[None], out_ref.shape)


def final_kernel(batches, toks, stats_ref, seq_ref, token_ref, mean_ref):
    member = lax.axis_index("expert")
    members = lax.axis_size("expert")
    sections = lax.axis_size("section")
    count = members * toks
    stats = stats_ref[:, 0, :]
    spot = member * toks
    lane = iota((1, count), 1)
    seat = iota((1, SEQS), 1)
    for m in range(batches):
        rows = [stats[s * members : (s + 1) * members] for s in range(m, sections, batches)]
        rows = rows[0] if len(rows) == 1 else jnp.concatenate(rows, 0)
        local, hits = rows[:, :count], rows[:, count:]
        peak = jnp.max(local, 0, keepdims=True)
        lse = peak + jnp.log(jnp.sum(jnp.exp(local - peak), 0, keepdims=True))
        logprob = jnp.sum(hits, 0, keepdims=True) - lse
        ids = seq_ref[m : m + 1, :]
        means = jnp.zeros((1, SEQS), F32)
        for s in range(SEQS):
            inside = ids == s
            summed = jnp.sum(jnp.where(inside, logprob, 0.0), 1, keepdims=True)
            size = jnp.sum(jnp.where(inside, 1.0, 0.0), 1, keepdims=True)
            means = jnp.where(seat == s, summed / size, means)
        mean_ref[m : m + 1, :] = means
        mine = pltpu.roll(logprob, count - spot, 1)
        token_ref[m : m + 1, :] = mine[:, :toks]


def body(
    hidden_in, layer_gain, router, w_gate, w_up, w_down, final_gain, head, routing, targets, seq_ids
):
    batches, toks, width = hidden_in.shape
    experts = router.shape[2]
    tops = routing.shape[3]
    sections = lax.axis_size("section")
    members = lax.axis_size("expert")
    splits = members // experts // PAIR
    groups = members // PAIR
    cap = min(toks, 9 * toks * tops // (8 * experts))
    dims = (batches, toks, width, experts, splits, tops, cap)
    same_core = [[g * PAIR + c for g in range(groups)] for c in range(PAIR)]
    same_core_all = [
        [s * members + g * PAIR + c for s in range(sections) for g in range(groups)]
        for c in range(PAIR)
    ]
    partner = [(i, i ^ 1) for i in range(members)]
    split = splits * PAIR
    same_place = [[e * split + r for e in range(experts)] for r in range(split)]
    same_place_all = [
        [s * members + e * split + r for s in range(sections) for e in range(experts)]
        for r in range(split)
    ]

    def exchange(rows):
        return lax.all_to_all(
            rows, "expert", split_axis=0, concat_axis=0, axis_index_groups=same_core, tiled=True
        )

    def exchange_all(rows, over):
        return lax.all_to_all(
            rows,
            ("section", "expert"),
            split_axis=0,
            concat_axis=0,
            axis_index_groups=over,
            tiled=True,
        )

    def dispatch_first(rows):
        return lax.all_to_all(
            rows, "expert", split_axis=0, concat_axis=0, axis_index_groups=same_place, tiled=True
        )

    def to_split(rows, shift):
        pairs = []
        for i in range(members):
            place = i // PAIR % splits
            pairs.append((i, i + ((place + shift) % splits - place) * PAIR))
        return lax.ppermute(rows, "expert", pairs)

    def swap_core(rows):
        return lax.ppermute(rows, "expert", partner)

    def by_section(array, shift, across):
        return lax.ppermute(
            array,
            "section",
            [(s, s - s % across + (s + shift) % across) for s in range(sections)],
        )

    early = head.shape[0] * 5 // 8 // 16 * 16
    table_rows = max(-(-(2 + experts) // 8) * 8, toks)
    packed, small, states, early_head = prep(
        dims, table_rows, early, hidden_in, layer_gain, router, routing, final_gain, head
    )
    first_parts = []
    for shift in range(1, batches):
        first_parts.append(by_section(early_head, shift, batches))
    near = dispatch_first(packed)

    shifted = [small]
    for shift in range(1, sections):
        shifted.append(by_section(small, shift, sections))

    inner_size = experts * HALVES * cap
    for tick in range(sections):
        crossing = []
        for shift in range(1, splits):
            crossing.append(to_split(near, shift))
        mixes, gain, *got = ready(dims, tick, sections, (w_gate[0], w_up[0], w_down[0]), head, early, states, shifted)
        pack = got.pop(0) if tick < sections - 1 else None
        weights = got[:3]
        if tick == 0:
            late_head = got[3]
        mine = [near, *crossing]
        sources = mine + [swap_core(rows) for rows in mine]
        keep, send = expert_rows(dims, tick, sources, weights)
        total = (keep.astype(F32) + swap_core(send).astype(F32)).astype(BF16)
        if sections > batches:
            total = jnp.concatenate([total] * (sections // batches), 0)
        back = exchange_all(total, same_core_all)
        if tick == sections - 1:
            break
        states, packed = advance(dims, tick, back, mixes, states, gain, pack)
        near = exchange_all(packed, same_place_all)
        if sections > batches:
            base = tick + 1 - (tick + 1) % batches
            near = near[base * inner_size : (base + batches) * inner_size]
        if tick == 0:
            near, late_head = lax.optimization_barrier((near, late_head))
            late_parts = []
            for shift in range(1, batches):
                late_parts.append(by_section(late_head, shift, batches))

    (last_rows,) = advance(dims, tick, back, mixes, states, gain, None)
    near = exchange(last_rows)
    far = swap_core(near)
    world = sections * members
    table = call(
        lambda *refs: table_kernel(batches, members * toks, *refs),
        [
            ((batches * head.shape[0], width), BF16, True),
            ((members * toks, members * toks), BF16),
            ((1, members * toks), jnp.int32),
        ],
        (targets, head, *first_parts, *late_parts),
        [VMEM, HBM] + [ANY] * (2 * batches - 2),
        [pltpu.SemaphoreType.DMA((2 * batches - 1,))],
    )
    (stats,) = call(
        lambda *refs: head_kernel(batches, early, *refs),
        [((world, 1, 2 * members * toks), F32)],
        (near, far, *table),
        [VMEM] * 5,
        flops=4 * head.size * members * toks,
    )
    stats = lax.all_to_all(stats, ("section", "expert"), split_axis=0, concat_axis=0, tiled=True)
    return call(
        lambda *refs: final_kernel(batches, toks, *refs),
        [((batches, toks), F32), ((batches, SEQS), F32)],
        (stats, seq_ids),
        [VMEM] * 2,
    )


def solution(mesh):
    return jax.shard_map(
        body,
        mesh=mesh,
        in_specs=(
            P(None, "expert", None),
            P("section", None),
            P("section", None, None),
            P("section", None, "expert"),
            P("section", None, "expert"),
            P("section", "expert", None),
            P(),
            P(("section", "expert"), None),
            P("section", None, "expert", None),
            P(),
            P(),
        ),
        out_specs=(P(None, "expert"), P()),
        check_vma=False,
    )
```
